256 devices in a mesh: section: 2 (over core), dp: 8 (over y_hi, x), tensor: 16 (over z, y_lo).
Axes of the slice: x: 4, y: 4 (y_hi: 2, y_lo: 2; y = y_hi * 2 + y_lo), z: 8, core: 2. Of those that a mesh axis runs over, the one named last changes fastest.
Arguments:
- tokens_in: bfloat16 [1024, 8192], P('dp', ('section', 'tensor')), may hold values from -70 to 70
- gain_attn: bfloat16 [8192], replicated, may hold values from 0.5 to 1.5
- w_query: bfloat16 [8192, 8192], P(None, ('section', 'tensor')), may hold values from -6 to 6
- w_keyval: bfloat16 [8192, 2048], P(None, ('section', 'tensor')), may hold values from -0.0625 to 0.0625
- w_out: bfloat16 [8192, 8192], P(('section', 'tensor')), may hold values from -0.0625 to 0.0625
- gain_mlp: bfloat16 [8192], replicated, may hold values from 0.5 to 1.5
- w_gate: bfloat16 [8192, 16384], P('dp', ('section', 'tensor')), may hold values from -0.0625 to 0.0625
- w_up: bfloat16 [8192, 16384], P('dp', ('section', 'tensor')), may hold values from -0.0625 to 0.0625
- w_down: bfloat16 [16384, 8192], P(('section', 'tensor'), 'dp'), may hold values from -0.046875 to 0.046875
Outputs:
- layer_out: bfloat16 [1024, 8192], P(('section', 'tensor'), 'dp')
The draws below stay inside these ranges and needn't reach their ends.
All inputs are finite; a program needn't handle non-finite values.
Results may differ from the reference program's by a relative error of at most 0.0068.
Values may be sent and summed in bfloat16 or wider, within the bound.
No kernel may reach another device: no remote copies, remote signals or barrier semaphores. Data moves between devices by JAX's collectives and lax.ppermute only.
A program may use at most 64 MiB of HBM per device.

```python
import math
import jax
import jax.numpy as jnp
from jax import lax

D = 8192
H = 64
KVH = 8
HD = 128
FF = 16384
TOKENS = 1024


def draw_tokens_in(key, part):
    first_key, scale_key = jax.random.split(jax.random.fold_in(key, 11), 2)
    base_values = jnp.clip(jax.random.normal(first_key, (TOKENS, D), jnp.float32), -6.0, 6.0)
    scales = jnp.exp(jax.random.uniform(scale_key, (TOKENS, 1), jnp.float32, math.log(0.3), math.log(3.0)))
    values = scales * base_values
    return values.astype(jnp.bfloat16)


def draw_w_query(key, part):
    entry_key, head_key = jax.random.split(jax.random.fold_in(key, 23), 2)
    base_values = jnp.clip(jax.random.normal(entry_key, (D, H * HD), jnp.float32), -6.0, 6.0) * D ** (-0.5)
    head_scale = jnp.exp(jax.random.uniform(head_key, (H,), jnp.float32, 0.0, math.log(3.0)))
    values = base_values * jnp.repeat(head_scale, HD)[None, :]
    values = jnp.clip(values, -6.0, 6.0)
    return values.astype(jnp.bfloat16)


def block_levels(own_key, extent, pieces, smallest, high):
    factor_of = 1.0
    for dim, parts in pieces:
        steps = jax.random.uniform(jax.random.fold_in(jax.random.fold_in(own_key, 6), dim), (parts,), jnp.float32, smallest / len(pieces), high / len(pieces))
        factor_of = factor_of * jnp.repeat(jnp.exp(steps), extent[dim] // parts).reshape((-1,) + (1,) * (len(extent) - 1 - dim))
    return factor_of


def noise(stream_key, dims, width, limit, shards=(), kind=jnp.bfloat16):
    entries = width * jax.random.normal(stream_key, dims, jnp.float32)
    if shards:
        entries = entries * block_levels(stream_key, dims, shards, -0.22, 0.18)
    return jnp.clip(entries, -limit, limit).astype(kind)


def setup_inputs(seed: int = 0) -> dict:
    arg_keys = jax.random.split(jax.random.key(seed), 10)
    tokens_in = draw_tokens_in(jax.random.fold_in(arg_keys[9], 71), 0)
    gain_attn = jnp.clip(1.0 + 0.1 * jax.random.normal(arg_keys[1], (D,), jnp.float32), 0.5, 1.5).astype(jnp.bfloat16)
    w_query = draw_w_query(jax.random.fold_in(arg_keys[9], 71), 0)
    w_keyval = noise(arg_keys[3], (D, 2 * KVH * HD), D ** -0.5, 0.0625, ((1, 32),))
    w_out = noise(arg_keys[4], (H * HD, D), (H * HD) ** -0.5, 0.0625, ((0, 32),))
    gain_mlp = jnp.clip(1.0 + 0.1 * jax.random.normal(arg_keys[5], (D,), jnp.float32), 0.5, 1.5).astype(jnp.bfloat16)
    w_gate = noise(arg_keys[6], (D, FF), D ** -0.5, 0.0625, ((0, 8), (1, 32)))
    w_up = noise(arg_keys[7], (D, FF), D ** -0.5, 0.0625, ((0, 8), (1, 32)))
    w_down = noise(arg_keys[8], (FF, D), FF ** -0.5, 0.046875, ((0, 32), (1, 8)))
    return {"tokens_in": tokens_in, "gain_attn": gain_attn, "w_query": w_query, "w_keyval": w_keyval, "w_out": w_out, "gain_mlp": gain_mlp, "w_gate": w_gate, "w_up": w_up, "w_down": w_down}


EPS = 1e-05
THETA = 10000.0

def rms_scale(row_data, gain_row):
    values = row_data.astype(jnp.float32)
    factor = lax.rsqrt(lax.optimization_barrier(jnp.mean(values * values, axis=-1, keepdims=True)) + EPS)
    return (values * factor * gain_row.astype(jnp.float32)).astype(jnp.bfloat16)

def rotary(values, positions):
    half_dim = values.shape[-1] // 2
    frequency = THETA ** (-jnp.arange(half_dim, dtype=jnp.float32) * 2.0 / values.shape[-1])
    angles = positions.astype(jnp.float32)[:, None] * frequency[None, :]
    cosine = jnp.cos(angles)[:, None, :]
    sine_part = jnp.sin(angles)[:, None, :]
    first_half = values[..., :half_dim]
    second = values[..., half_dim:]
    return jnp.concatenate([first_half * cosine - second * sine_part, second * cosine + first_half * sine_part], axis=-1)

def reference(tokens_in, gain_attn, w_query, w_keyval, w_out, gain_mlp, w_gate, w_up, w_down):
    total_rows = tokens_in.shape[0]
    normed_attn = rms_scale(tokens_in, gain_attn)
    positions = jnp.arange(total_rows, dtype=jnp.int32)
    query_proj = jnp.dot(normed_attn, w_query, preferred_element_type=jnp.float32)
    query_rot = rotary(query_proj.reshape(total_rows, H, HD), positions).astype(jnp.bfloat16)
    keyval = jnp.dot(normed_attn, w_keyval, preferred_element_type=jnp.float32).astype(jnp.bfloat16)
    key_rot = rotary(keyval[:, :KVH * HD].astype(jnp.float32).reshape(total_rows, KVH, HD), positions).astype(jnp.bfloat16)
    value_all = keyval[:, KVH * HD:].reshape(total_rows, KVH, HD)
    group_size = H // KVH
    query_grp = query_rot.reshape(total_rows, KVH, group_size, HD)
    allowed = positions[None, :] <= positions[:, None]

    def one_group(operands):
        q_block, k_block, v_block = operands
        scores = jnp.einsum('rgd,sd->grs', q_block.astype(jnp.float32), k_block.astype(jnp.float32)) * HD ** (-0.5)
        scores = jnp.where(allowed[None, :, :], scores, -1e+30)
        row_peak = lax.optimization_barrier(jnp.max(scores, axis=-1, keepdims=True))
        expo = jnp.exp(scores - row_peak)
        prob_rows = (expo / lax.optimization_barrier(jnp.sum(expo, axis=-1, keepdims=True))).astype(jnp.bfloat16)
        mixed = jnp.einsum('grs,sd->rgd', prob_rows.astype(jnp.float32), v_block.astype(jnp.float32))
        return mixed.astype(jnp.bfloat16)
    attended = lax.map(one_group, (jnp.transpose(query_grp, (1, 0, 2, 3)), jnp.transpose(key_rot, (1, 0, 2)), jnp.transpose(value_all, (1, 0, 2))))
    attended = jnp.transpose(attended, (1, 0, 2, 3)).reshape(total_rows, H * HD)
    head_sum = jnp.dot(attended, w_out, preferred_element_type=jnp.float32)
    mid_rows = (tokens_in.astype(jnp.float32) + head_sum).astype(jnp.bfloat16)
    normed_mlp = rms_scale(mid_rows, gain_mlp)
    gate_sum = jnp.dot(normed_mlp, w_gate, preferred_element_type=jnp.float32)
    up_sum = jnp.dot(normed_mlp, w_up, preferred_element_type=jnp.float32)
    hidden = (jax.nn.silu(gate_sum) * up_sum).astype(jnp.bfloat16)
    down_sum = jnp.dot(hidden, w_down, preferred_element_type=jnp.float32)
    return (mid_rows.astype(jnp.float32) + down_sum).astype(jnp.bfloat16)
```

```python
import jax
import jax.numpy as jnp
from jax import lax
from jax.sharding import Mesh
from jax.sharding import PartitionSpec as P

H = 64
KVH = 8
HD = 128
EPS = 1e-05
THETA = 10000.0

F32 = jnp.float32
BF16 = jnp.bfloat16
DP = ("yh", "x")
Z = ("zh", "zl")
GROUP = ("c", "zh", "zl", "yl")
SWAP = [(0, 1), (1, 0)]


def dot(a, b):
    return jnp.dot(a, b, preferred_element_type=F32)


def to_all(array, axis):
    length = lax.axis_size(axis)
    return lax.all_to_all(
        jnp.broadcast_to(array[None], (length, *array.shape)), axis, 0, 0, tiled=True
    )


def exchange(tiles, axis):
    return lax.all_to_all(tiles, axis, 0, 0, tiled=True)


def rope_tables(positions):
    half = HD // 2
    frequency = THETA ** (-jnp.arange(half, dtype=F32) * 2.0 / HD)
    angles = positions.astype(F32)[:, None] * frequency[None, :]
    return jnp.cos(angles), jnp.sin(angles)


def shards(tokens_in, gain_attn, w_query, w_keyval, w_out, gain_mlp, w_gate, w_up, w_down):
    core = lax.axis_index("c")
    block = lax.axis_index(DP)
    z_lo = lax.axis_index("zl")
    y_lo = lax.axis_index("yl")
    rows, width = tokens_in.shape
    n_dp = lax.axis_size(DP)
    n_z = lax.axis_size(Z)
    half_d = w_query.shape[0] // 2
    total = rows * n_dp

    pair = to_all(tokens_in, "yl")
    own = to_all(pair, Z).reshape(2 * n_z, rows, width)
    other = lax.ppermute(own, "c", SWAP)

    def flat(pieces):
        return jnp.moveaxis(pieces, 0, 1).reshape(rows, half_d)

    own_rows, other_rows = flat(own), flat(other)
    parts = ((own_rows, core), (other_rows, 1 - core))
    square = sum(jnp.sum(jnp.square(r.astype(F32)), axis=-1, keepdims=True) for r, _ in parts)
    factor = lax.rsqrt(square / (2 * half_d) + EPS)

    def project(weight):
        out = 0.0
        for r, k in parts:
            gain = lax.dynamic_slice_in_dim(gain_attn, k * half_d, half_d, 0)
            normed = (r.astype(F32) * factor * gain.astype(F32)[None, :]).astype(BF16)
            out = out + dot(normed, lax.dynamic_slice_in_dim(weight, k * half_d, half_d, 0))
        return out

    kv_part = project(w_keyval).astype(BF16).T
    n_group = lax.axis_size(GROUP)
    moves = []
    for g in range(n_group):
        c, z, y = g // (2 * n_z), (g // 2) % n_z, g % 2
        moves.append((g, (z // 4) * 2 * n_z + (2 * (z % 4) + c) * 2 + y))
    kv_here = lax.ppermute(kv_part, GROUP, moves)
    kv_all = to_all(kv_here, ("yh", "x", "zl", "yl")).reshape(n_dp, 2, HD, rows)
    key_t = jnp.moveaxis(kv_all[:, 0], 0, 1).reshape(HD, total)
    value_t = jnp.moveaxis(kv_all[:, 1], 0, 1).reshape(HD, total)
    key_pos = jnp.arange(total, dtype=jnp.int32)
    cos_k, sin_k = rope_tables(key_pos)
    cos_k, sin_k = cos_k.T, sin_k.T
    k1, k2 = key_t[: HD // 2].astype(F32), key_t[HD // 2 :].astype(F32)
    key_rot = jnp.concatenate(
        [k1 * cos_k - k2 * sin_k, k2 * cos_k + k1 * sin_k], axis=0
    ).astype(BF16)

    pos = block * rows + jnp.arange(rows, dtype=jnp.int32)
    cos_q, sin_q = rope_tables(pos)
    query = project(w_query)
    heads = w_query.shape[1] // HD
    q_rot = []
    for h in range(heads):
        q1 = query[:, h * HD : h * HD + HD // 2]
        q2 = query[:, h * HD + HD // 2 : (h + 1) * HD]
        q_rot.append(
            jnp.concatenate([q1 * cos_q - q2 * sin_q, q2 * cos_q + q1 * sin_q], axis=1)
        )
    q_rot = jnp.concatenate(q_rot, axis=0).astype(BF16)
    scores = dot(q_rot, key_rot) * HD ** (-0.5)
    allowed = key_pos[None, :] <= jnp.tile(pos, heads)[:, None]
    scores = jnp.where(allowed, scores, -1e30)
    expo = jnp.exp(scores - jnp.max(scores, axis=-1, keepdims=True))
    probs = (expo / jnp.sum(expo, axis=-1, keepdims=True)).astype(BF16)
    attended = lax.dot_general(
        probs, value_t, (((1,), (1,)), ((), ())), preferred_element_type=F32
    ).astype(BF16)
    attended = jnp.concatenate([attended[h * rows : (h + 1) * rows] for h in range(heads)], axis=1)

    def out_half(k):
        return dot(attended, lax.dynamic_slice_in_dim(w_out, k * half_d, half_d, 1))

    sent = lax.ppermute(out_half(1 - core).astype(BF16), "c", SWAP)
    terms = (out_half(core) + sent.astype(F32)).astype(BF16)
    block_d = half_d // 4
    tiles = terms.reshape(2, rows // 2, 4, block_d).transpose(2, 0, 1, 3)
    tiles = exchange(tiles.reshape(n_z, rows // 2, block_d), Z)
    terms = tiles.astype(F32).sum(axis=0).astype(BF16)
    tiles = exchange(terms.reshape(2, rows // 4, block_d), "yl")
    z_hi = lax.axis_index("zh")
    resid = lax.dynamic_slice(
        own_rows, ((z_lo * 2 + y_lo) * (rows // 4), z_hi * block_d), (rows // 4, block_d)
    )
    mid_part = (resid.astype(F32) + tiles.astype(F32).sum(axis=0)).astype(BF16)

    every = ("c", "yh", "x", "zh", "zl", "yl")
    moves = []
    for c in range(2):
        for d in range(n_dp):
            for z in range(n_z):
                for y in range(2):
                    source = ((c * n_dp + d) * n_z + z) * 2 + y
                    d2, g2 = c * 4 + z // 2, 4 * d + (z % 2) * 2 + y
                    c2, z2, y2 = g2 // (2 * n_z), (g2 // 2) % n_z, g2 % 2
                    moves.append((source, ((c2 * n_dp + d2) * n_z + z2) * 2 + y2))
    resid_rows = lax.ppermute(mid_part, every, moves)

    pair = to_all(resid_rows, "yl")
    mine = to_all(pair, Z).reshape(total // 2, block_d)
    theirs = lax.ppermute(mine, "c", SWAP)
    first = jnp.where(core == 0, mine, theirs)
    second = jnp.where(core == 0, theirs, mine)
    mid_cols = jnp.concatenate([first, second], axis=0)
    gain_cols = lax.dynamic_slice_in_dim(gain_mlp, block * block_d, block_d, 0).astype(F32)
    mid_f32 = mid_cols.astype(F32)
    square = jnp.sum(jnp.square(mid_f32), axis=-1)
    lhs = (mid_f32 * gain_cols[None, :]).astype(BF16)
    hidden_width = w_gate.shape[1]
    gate_up = jnp.concatenate([dot(lhs, w_gate), dot(lhs, w_up)], axis=1).astype(BF16)
    top = square.astype(BF16)
    low = (square - top.astype(F32)).astype(BF16)
    extra = jnp.concatenate([top.reshape(n_dp, 1, rows), low.reshape(n_dp, 1, rows)], axis=2)
    extra = jnp.pad(extra, ((0, 0), (0, 7), (0, 2 * hidden_width - 2 * rows)))
    tiles = jnp.concatenate([gate_up.reshape(n_dp, rows, 2 * hidden_width), extra], axis=1)
    tiles = exchange(tiles, DP).astype(F32).sum(axis=0)
    square = tiles[rows, :rows] + tiles[rows, rows : 2 * rows]
    scale = lax.rsqrt(square / (2 * half_d) + EPS)[:, None]
    gate = tiles[:rows, :hidden_width] * scale
    up = tiles[:rows, hidden_width:] * scale
    hidden = (jax.nn.silu(gate) * up).astype(BF16)

    hidden_all = to_all(hidden, DP).reshape(total, hidden_width)

    def down_half(k):
        return dot(lax.dynamic_slice_in_dim(hidden_all, k * (total // 2), total // 2, 0), w_down)

    sent = lax.ppermute(down_half(1 - core).astype(BF16), "c", SWAP)
    terms = (down_half(core) + sent.astype(F32)).astype(BF16)
    tiles = exchange(terms.reshape(n_z, total // 2 // n_z, block_d), Z)
    terms = tiles.astype(F32).sum(axis=0).astype(BF16)
    tiles = exchange(terms.reshape(2, rows // 4, block_d), "yl")
    return (resid_rows.astype(F32) + tiles.astype(F32).sum(axis=0)).astype(BF16)


def solution(mesh):
    fine = Mesh(
        mesh.devices.reshape(2, 2, 4, 4, 2, 2), ("c", "yh", "x", "zh", "zl", "yl")
    )
    placed = (
        P(DP, GROUP),
        P(),
        P(None, GROUP),
        P(None, GROUP),
        P(GROUP, None),
        P(),
        P(DP, GROUP),
        P(DP, GROUP),
        P(GROUP, DP),
    )
    return jax.shard_map(
        shards, mesh=fine, in_specs=placed, out_specs=P(GROUP, DP), check_vma=False
    )
```

```python
import jax
import jax.numpy as jnp
from jax import lax
from jax.sharding import Mesh
from jax.sharding import PartitionSpec as P


HD = 128
EPS = 1e-05
THETA = 10000.0

F32 = jnp.float32
BF16 = jnp.bfloat16
DP = ("yh", "x")
Z = ("zh", "zl")
GROUP = ("c", "zh", "zl", "yl")
EVERY = ("c", "yh", "x", "zh", "zl", "yl")
SIZES = (2, 2, 4, 4, 2, 2)
SWAP = [(0, 1), (1, 0)]
NX = 4


def dot(a, b):
    return jnp.dot(a, b, preferred_element_type=F32)


def to_all(array, axis):
    length = lax.axis_size(axis)
    return lax.all_to_all(
        jnp.broadcast_to(array[None], (length, *array.shape)), axis, 0, 0, tiled=True
    )


def exchange(tiles, axis):
    return lax.all_to_all(tiles, axis, 0, 0, tiled=True)


def trade(array, first, second):
    i, j = EVERY.index(first), EVERY.index(second)
    moves = []
    for n in range(256):
        at, rest = [], n
        for size in reversed(SIZES):
            at.append(rest % size)
            rest //= size
        at.reverse()
        at[i], at[j] = at[j], at[i]
        to = 0
        for place, size in zip(at, SIZES):
            to = to * size + place
        moves.append((n, to))
    return lax.ppermute(array, EVERY, moves)


def rope_tables(positions):
    half = HD // 2
    frequency = THETA ** (-jnp.arange(half, dtype=F32) * 2.0 / HD)
    angles = positions.astype(F32)[:, None] * frequency[None, :]
    return jnp.cos(angles), jnp.sin(angles)


def pick(array, index, axis=0):
    return lax.dynamic_index_in_dim(array, index, axis, keepdims=False)


def along_x(array):
    return [array] + [
        lax.ppermute(array, "x", [(i, (i - r) % NX) for i in range(NX)]) for r in range(1, NX)
    ]


def layer(tokens_in, gain_attn, w_query, w_keyval, w_out, gain_mlp, w_gate, w_up, w_down):
    core, y_hi, x = lax.axis_index("c"), lax.axis_index("yh"), lax.axis_index("x")
    z_hi, z_lo, y_lo = lax.axis_index("zh"), lax.axis_index("zl"), lax.axis_index("yl")
    block = lax.axis_index(DP)
    rows, width = tokens_in.shape
    n_dp, n_z = lax.axis_size(DP), lax.axis_size(Z)
    dim = w_query.shape[0]
    half_d, block_d = dim // 2, dim // 8
    total = rows * n_dp
    quarter = rows // 4
    hid = w_gate.shape[1]

    gain_cols = lax.dynamic_slice_in_dim(gain_mlp, block * block_d, block_d, 0)
    gate_up_w = jnp.concatenate([w_gate, w_up], axis=1).astype(F32)
    gate_up_w = (gate_up_w * gain_cols.astype(F32)[:, None]).astype(BF16)

    gate_up_all = along_x(gate_up_w)
    down_all = along_x(w_down)

    own = to_all(tokens_in, Z)
    own_c = lax.ppermute(own, "c", SWAP)
    far = lax.ppermute(own, "yl", SWAP)
    far_c = lax.ppermute(far, "c", SWAP)
    parts = ((own, 0, 0), (own_c, 1, 0), (far, 0, 1), (far_c, 1, 1))

    def gained(weight):
        out = (weight.astype(F32) * gain_attn.astype(F32)[:, None]).astype(BF16)
        return out.reshape(2, n_z, 2, width, weight.shape[1])

    scaled = [gained(w_query), gained(w_keyval)]
    square, out = 0.0, [0.0, 0.0]
    for piece, rc, ry in parts:
        at = (core ^ rc, 0, y_lo ^ ry, 0, 0)
        piece = piece.transpose(1, 0, 2).reshape(rows, n_z * width)
        square = square + jnp.sum(jnp.square(piece.astype(F32)), axis=1)
        for i, weight in enumerate(scaled):
            n = weight.shape[-1]
            weight = lax.dynamic_slice(weight, at, (1, n_z, 1, width, n))
            out[i] = out[i] + dot(piece, weight.reshape(n_z * width, n))
    factor = lax.rsqrt(square / dim + EPS)[:, None]
    query, kv_part = out[0] * factor, out[1] * factor

    n_group = lax.axis_size(GROUP)
    moves = []
    for g in range(n_group):
        c, z, y = g // (2 * n_z), (g // 2) % n_z, g % 2
        moves.append((g, (z // 4) * 2 * n_z + (2 * (z % 4) + c) * 2 + y))
    kv_here = lax.ppermute(kv_part.astype(BF16).T, GROUP, moves)
    kv_all = to_all(kv_here, ("yh", "x", "zl", "yl")).reshape(n_dp, 2, HD, rows)
    key_t = jnp.moveaxis(kv_all[:, 0], 0, 1).reshape(HD, total)
    value_t = jnp.moveaxis(kv_all[:, 1], 0, 1).reshape(HD, total)

    key_pos = jnp.arange(total, dtype=jnp.int32)
    cos_k, sin_k = rope_tables(key_pos)
    cos_k, sin_k = cos_k.T, sin_k.T
    k1, k2 = key_t[: HD // 2].astype(F32), key_t[HD // 2 :].astype(F32)
    key_rot = jnp.concatenate(
        [k1 * cos_k - k2 * sin_k, k2 * cos_k + k1 * sin_k], axis=0
    ).astype(BF16)
    pos = block * rows + jnp.arange(rows, dtype=jnp.int32)
    cos_q, sin_q = rope_tables(pos)
    heads = w_query.shape[1] // HD
    q_rot = []
    for h in range(heads):
        q1 = query[:, h * HD : h * HD + HD // 2]
        q2 = query[:, h * HD + HD // 2 : (h + 1) * HD]
        q_rot.append(jnp.concatenate([q1 * cos_q - q2 * sin_q, q2 * cos_q + q1 * sin_q], axis=1))
    q_rot = jnp.concatenate(q_rot, axis=0).astype(BF16)
    scores = dot(q_rot, key_rot) * HD ** (-0.5)
    allowed = key_pos[None, :] <= jnp.tile(pos, heads)[:, None]
    scores = jnp.where(allowed, scores, -1e30)
    expo = jnp.exp(scores - jnp.max(scores, axis=-1, keepdims=True))
    probs = (expo / jnp.sum(expo, axis=-1, keepdims=True)).astype(BF16)
    attended = lax.dot_general(
        probs, value_t, (((1,), (1,)), ((), ())), preferred_element_type=F32
    ).astype(BF16)
    attended = jnp.concatenate([attended[h * rows : (h + 1) * rows] for h in range(heads)], axis=1)

    def out_half(k):
        return dot(attended, lax.dynamic_slice_in_dim(w_out, k * half_d, half_d, 1))

    sent = lax.ppermute(out_half(1 - core).astype(BF16), "c", SWAP)
    terms = (out_half(core) + sent.astype(F32)).astype(BF16)
    terms = terms.reshape(2, 2, quarter, half_d)
    sent = lax.ppermute(pick(terms, 1 - y_lo, 1), "yl", SWAP)
    terms = (pick(terms, y_lo, 1).astype(F32) + sent.astype(F32)).astype(BF16)
    tiles = terms.reshape(2, quarter, 4, block_d).transpose(2, 0, 1, 3)
    tiles = exchange(tiles.reshape(n_z, quarter, block_d), Z)
    near = own.reshape(4, 2, rows, width)
    far_near = far.reshape(4, 2, rows, width)
    start = (z_lo * 2 + y_lo) * quarter
    mine = lax.dynamic_slice(near, (z_hi, 0, start, 0), (1, 2, quarter, width))[0]
    other = lax.dynamic_slice(far_near, (z_hi, 0, start, 0), (1, 2, quarter, width))[0]
    low = jnp.where(y_lo == 0, mine, other)
    high = jnp.where(y_lo == 0, other, mine)
    resid = jnp.stack([low, high], axis=1).transpose(2, 0, 1, 3).reshape(quarter, block_d)
    mid_part = (resid.astype(F32) + tiles.astype(F32).sum(axis=0)).astype(BF16)
    mid_own = trade(mid_part, "yh", "c")

    near = to_all(mid_own, Z).reshape(4, 2 * quarter, block_d)
    near_c = lax.ppermute(near, "c", SWAP)
    far = lax.ppermute(near, "yl", SWAP)
    far_c = lax.ppermute(far, "c", SWAP)
    mids = jnp.stack(
        [jnp.concatenate([near, far], axis=1), jnp.concatenate([near_c, far_c], axis=1)], axis=0
    )

    def gate_up(rc):
        lhs = pick(mids, rc)
        out = 0.0
        for r in range(NX):
            out = out + dot(pick(lhs, (x + r) % NX), gate_up_all[r])
        square = jnp.sum(jnp.square(lhs.astype(F32)), axis=(0, 2))
        return out, square

    out, square = gate_up((1 - y_hi) ^ core)
    top = square.astype(BF16)
    low = (square - top.astype(F32)).astype(BF16)
    extra = jnp.pad(
        jnp.concatenate([top, low])[None], ((0, 15), (0, 2 * hid - 2 * rows))
    )
    sent = lax.ppermute(jnp.concatenate([out.astype(BF16), extra], axis=0), "yh", SWAP)
    out, square = gate_up(y_hi ^ core)
    sent = sent.astype(F32)
    out = out + sent[:rows]
    square = square + sent[rows, :rows] + sent[rows, rows : 2 * rows]
    out = out * lax.rsqrt(square / dim + EPS)[:, None]
    hidden = (jax.nn.silu(out[:, :hid]) * out[:, hid:]).astype(BF16)

    other = lax.ppermute(hidden, "yh", SWAP)
    keep = jnp.where(y_hi == core, hidden, other)
    give = jnp.where(y_hi == core, other, hidden)
    down = jnp.stack(down_all, axis=0)

    def down_of(lhs):
        return [dot(lhs, pick(down, (k - x) % NX)) for k in range(NX)]

    sent = jnp.stack([t.astype(BF16) for t in down_of(give)], axis=0)
    sent = lax.ppermute(sent, "c", SWAP)
    terms = jnp.stack(down_of(keep), axis=0)
    terms = (terms + sent.astype(F32)).astype(BF16).reshape(NX, 2, 2 * quarter, block_d)
    sent = lax.ppermute(terms[:, 1], "yl", SWAP)
    tiles = (terms[:, 0].astype(F32) + sent.astype(F32)).astype(BF16)
    tiles = exchange(tiles.reshape(n_z, quarter, block_d), Z)
    done = (mid_own.astype(F32) + tiles.astype(F32).sum(axis=0)).astype(BF16)
    return trade(done, "x", "zh")


def solution(mesh):
    fine = Mesh(mesh.devices.reshape(SIZES), EVERY)
    placed = (
        P(DP, GROUP),
        P(),
        P(None, GROUP),
        P(None, GROUP),
        P(GROUP, None),
        P(),
        P(DP, GROUP),
        P(DP, GROUP),
        P(GROUP, DP),
    )
    return jax.shard_map(layer, mesh=fine, in_specs=placed, out_specs=P(GROUP, DP), check_vma=False)
```

```python
import jax
import jax.numpy as jnp
from jax import lax
from jax.experimental import pallas as pl
from jax.experimental.pallas import tpu as pltpu
from jax.sharding import Mesh
from jax.sharding import PartitionSpec as P


HD = 128
EPS = 1e-05
THETA = 10000.0

F32 = jnp.float32
BF16 = jnp.bfloat16
DP = ("yh", "x")
Z = ("zh", "zl")
GROUP = ("c", "zh", "zl", "yl")
EVERY = ("c", "yh", "x", "zh", "zl", "yl")
SIZES = (2, 2, 4, 4, 2, 2)
SWAP = [(0, 1), (1, 0)]
NX = 4


def dot(a, b):
    return jnp.dot(a, b, preferred_element_type=F32)


def dot_t(a, b):
    return lax.dot_general(a, b, (((1,), (1,)), ((), ())), preferred_element_type=F32)


def to_all(array, axis):
    length = lax.axis_size(axis)
    return lax.all_to_all(
        jnp.broadcast_to(array[None], (length, *array.shape)), axis, 0, 0, tiled=True
    )


def exchange(tiles, axis):
    return lax.all_to_all(tiles, axis, 0, 0, tiled=True)


def move(array, target):
    moves = []
    for n in range(256):
        at, rest = {}, n
        for name, size in zip(reversed(EVERY), reversed(SIZES)):
            at[name] = rest % size
            rest //= size
        goal, to = {**at, **target(**at)}, 0
        for name, size in zip(EVERY, SIZES):
            to = to * size + goal[name]
        moves.append((n, to))
    return lax.ppermute(array, EVERY, moves)


VMEM = pl.BlockSpec(memory_space=pltpu.VMEM)
SMEM = pl.BlockSpec(memory_space=pltpu.SMEM)
HBM = pl.BlockSpec(memory_space=pl.ANY)


def out_terms(place, attended, w_out, give):
    rows, depth = attended.shape
    block = w_out.shape[1] // (2 * NX)

    def body(place_ref, lhs_ref, w_hbm, out_ref, w, sem):
        half = 1 - place_ref[0] if give else place_ref[0]

        def copy(k):
            at = (half * NX + (place_ref[2] + k) % NX) * block
            return pltpu.make_async_copy(w_hbm.at[:, pl.ds(at, block)], w.at[k], sem.at[k])

        for k in range(NX):
            copy(k).start()
        for k in range(NX):
            copy(k).wait()
            out_ref[k] = dot(lhs_ref[...], w[k]).astype(out_ref.dtype)

    return pl.pallas_call(
        body,
        out_shape=jax.ShapeDtypeStruct((NX, rows, block), BF16 if give else F32),
        in_specs=[SMEM, VMEM, HBM],
        out_specs=VMEM,
        scratch_shapes=[
            pltpu.VMEM((NX, depth, block), BF16),
            pltpu.SemaphoreType.DMA((NX,)),
        ],
        name="out_give" if give else "out_keep",
    )(place, attended, w_out)


def gate_up_terms(place, pieces, weights):
    n, part, depth = pieces[0].shape
    rows, cols = 2 * part, weights[0].shape[1]

    def body(place_ref, *refs):
        pieces, weights, (give_ref, keep_ref, square_ref) = refs[:4], refs[4:8], refs[8:11]
        w, acc, sq, sem = refs[11:]
        copies = [
            pltpu.make_async_copy(weights[k], w.at[k], sem.at[k]) for k in range(n)
        ]
        for copy in copies:
            copy.start()
        for k in range(n):
            lhs = jnp.concatenate([p[k] for p in pieces], axis=0)
            wide = lhs.astype(F32)
            square = jnp.sum(wide * wide, axis=1, keepdims=True)
            copies[k].wait()
            out = dot(lhs, w[k])
            if k == 0:
                acc[...], sq[...] = out, jnp.broadcast_to(square, sq.shape)
            else:
                acc[...] += out
                sq[...] += square
        keep = pl.multiple_of((place_ref[3] ^ place_ref[0]) * rows, rows)
        give = pl.multiple_of(((1 - place_ref[3]) ^ place_ref[0]) * rows, rows)
        give_ref[:, :cols] = acc[pl.ds(give, rows)].astype(BF16)
        square = sq[pl.ds(give, rows)]
        top = square.astype(BF16)
        low = (square - top.astype(F32)).astype(BF16)
        lane = lax.broadcasted_iota(jnp.int32, square.shape, 1)
        give_ref[:, cols:] = jnp.where(lane == 0, top.astype(F32), low.astype(F32)).astype(BF16)
        keep_ref[...] = acc[pl.ds(keep, rows)]
        square_ref[...] = sq[pl.ds(keep, rows)]

    return pl.pallas_call(
        body,
        out_shape=[
            jax.ShapeDtypeStruct((rows, cols + 128), BF16),
            jax.ShapeDtypeStruct((rows, cols), F32),
            jax.ShapeDtypeStruct((rows, 128), F32),
        ],
        in_specs=[SMEM] + [VMEM] * 4 + [HBM] * 4,
        out_specs=[VMEM] * 3,
        scratch_shapes=[
            pltpu.VMEM((n, depth, cols), BF16),
            pltpu.VMEM((2 * rows, cols), F32),
            pltpu.VMEM((2 * rows, 128), F32),
            pltpu.SemaphoreType.DMA((n,)),
        ],
        name="gate_up",
    )(place, *pieces, *weights)


def hidden_units(keep, square, sent, dim):
    rows, cols = keep.shape

    def body(keep_ref, square_ref, sent_ref, out_ref):
        extra = sent_ref[:, cols:].astype(F32)
        mean = (square_ref[:, :1] + extra[:, :1] + extra[:, 1:2]) / dim
        out = (keep_ref[...] + sent_ref[:, :cols].astype(F32)) * lax.rsqrt(mean + EPS)
        gate, up = out[:, : cols // 2], out[:, cols // 2 :]
        out_ref[...] = (gate / (1.0 + jnp.exp(-gate)) * up).astype(BF16)

    return pl.pallas_call(
        body,
        out_shape=jax.ShapeDtypeStruct((rows, cols // 2), BF16),
        in_specs=[VMEM] * 3,
        out_specs=VMEM,
        name="hidden",
    )(keep, square, sent)


def down_terms(place, hidden, other, weights, give):
    n, rows = len(weights), hidden.shape[0]
    depth, cols = weights[0].shape

    def body(place_ref, hidden_ref, other_ref, *refs):
        weights, out_ref, w, sem = refs[:n], refs[n], refs[n + 1], refs[n + 2]
        copies = [
            pltpu.make_async_copy(weights[k], w.at[k], sem.at[k]) for k in range(n)
        ]
        for copy in copies:
            copy.start()
        same = place_ref[0] == place_ref[3]
        own = jnp.logical_not(same) if give else same
        lhs = jnp.where(own, hidden_ref[...], other_ref[...])
        for k in range(n):
            copies[k].wait()
            out_ref[k] = dot(lhs, w[k]).astype(out_ref.dtype)

    return pl.pallas_call(
        body,
        out_shape=jax.ShapeDtypeStruct((n, rows, cols), BF16 if give else F32),
        in_specs=[SMEM, VMEM, VMEM] + [HBM] * n,
        out_specs=VMEM,
        scratch_shapes=[pltpu.VMEM((n, depth, cols), BF16), pltpu.SemaphoreType.DMA((n,))],
        name="down_give" if give else "down_keep",
    )(place, hidden, other, *weights)


def rope_tables(positions):
    half = HD // 2
    frequency = THETA ** (-jnp.arange(half, dtype=F32) * 2.0 / HD)
    angles = positions.astype(F32)[:, None] * frequency[None, :]
    return jnp.cos(angles), jnp.sin(angles)


def pick(array, index, axis=0):
    return lax.dynamic_index_in_dim(array, index, axis, keepdims=False)


def from_x(array, r):
    return lax.ppermute(array, "x", [(i, (i - r) % NX) for i in range(NX)])


def project(place, near, near_c, gains, w_query, w_keyval, last, sums):
    n_z, rows, width = near.shape
    n_q, n_kv = w_query.shape[1], w_keyval.shape[0]
    steps = 2 * n_z

    def body(place_ref, near_ref, near_c_ref, gain_ref, wq_hbm, wkv_hbm, *refs):
        before, refs = (refs[:3], refs[3:]) if last else (None, refs)
        q_ref, kv_ref = refs[:2]
        sq_ref, wq, wkv, sem_q, sem_kv = refs[2:]
        core, y_lo = place_ref[0], place_ref[1] ^ (1 if last else 0)

        def at(i):
            half = core ^ 1 if i >= n_z else core
            return (half * n_z + i % n_z) * 2 + y_lo

        def copies(i):
            g = at(i) * width
            return (
                pltpu.make_async_copy(wq_hbm.at[pl.ds(g, width)], wq.at[i], sem_q.at[i]),
                pltpu.make_async_copy(wkv_hbm.at[:, pl.ds(g, width)], wkv.at[i], sem_kv.at[i]),
            )

        for i in range(steps):
            for copy in copies(i):
                copy.start()
        for i in range(steps):
            piece = (near_ref if i < n_z else near_c_ref)[i % n_z].astype(F32)
            lhs = (piece * gain_ref[at(i)]).astype(BF16)
            square = piece * piece
            for copy in copies(i):
                copy.wait()
            q, kv = dot(lhs, wq[i]), dot_t(wkv[i], lhs)
            if i == 0 and not last:
                sq_ref[...], q_ref[...], kv_ref[...] = square, q, kv
            elif i == 0:
                sq_ref[...] = before[2][...] + square
                q_ref[...] = before[0][...] + q
                kv_ref[...] = before[1][...] + kv
            else:
                sq_ref[...] += square
                q_ref[...] += q
                kv_ref[...] += kv
        if last:
            mean = jnp.sum(sq_ref[...], axis=1, keepdims=True) / (4 * n_z * width)
            factor = lax.rsqrt(mean + EPS)
            q_ref[...] = q_ref[...] * factor
            across = jnp.broadcast_to(factor, (rows, rows)).T[:1]
            kv_ref[...] = kv_ref[...] * across

    shapes = [(rows, n_q), (n_kv, rows), (rows, width)]
    shapes = [jax.ShapeDtypeStruct(shape, F32) for shape in shapes]
    scratch = [
        pltpu.VMEM((steps, width, n_q), BF16),
        pltpu.VMEM((steps, n_kv, width), BF16),
        pltpu.SemaphoreType.DMA((steps,)),
        pltpu.SemaphoreType.DMA((steps,)),
    ]
    if last:
        scratch = [pltpu.VMEM((rows, width), F32), *scratch]
    return pl.pallas_call(
        body,
        out_shape=shapes[: 2 if last else 3],
        in_specs=[SMEM, VMEM, VMEM, VMEM, HBM, HBM]
        + [VMEM] * (3 if last else 0),
        out_specs=[VMEM] * (2 if last else 3),
        scratch_shapes=scratch,
        name="project_last" if last else "project_first",
    )(place, near, near_c, gains, w_query, w_keyval, *(sums or ()))


def layer(tokens_in, gain_attn, w_query, w_keyval, w_out, gain_mlp, w_gate, w_up, w_down):
    core, y_hi, x = lax.axis_index("c"), lax.axis_index("yh"), lax.axis_index("x")
    z_hi, z_lo, y_lo = lax.axis_index("zh"), lax.axis_index("zl"), lax.axis_index("yl")
    block = lax.axis_index(DP)
    rows, width = tokens_in.shape
    n_dp, n_z = lax.axis_size(DP), lax.axis_size(Z)
    dim = w_query.shape[0]
    block_d = dim // 8
    total = rows * n_dp
    quarter = rows // 4

    gain_cols = lax.dynamic_slice_in_dim(gain_mlp, block * block_d, block_d, 0)
    gate_up_w = jnp.concatenate([w_gate, w_up], axis=1).astype(F32)
    gate_up_w = (gate_up_w * gain_cols.astype(F32)[:, None]).astype(BF16)

    gate_up_next, gate_up_last = from_x(gate_up_w, 1), from_x(gate_up_w, 3)
    gate_up_all = [gate_up_w, gate_up_next, from_x(gate_up_w, 2), gate_up_last]
    down_all = [w_down] + [from_x(w_down, r) for r in range(1, NX)]

    own = to_all(tokens_in, Z)
    own_c = lax.ppermute(own, "c", SWAP)
    far_rows = lax.ppermute(own, "yl", SWAP)
    far_c = lax.ppermute(far_rows, "c", SWAP)
    place = jnp.stack([core, y_lo, x, y_hi]).astype(jnp.int32)
    gains = gain_attn.astype(F32).reshape(2 * n_z * 2, 1, width)
    sums = project(place, own, own_c, gains, w_query, w_keyval.T, False, None)
    query, kv_part = project(place, far_rows, far_c, gains, w_query, w_keyval.T, True, sums)

    n_group = lax.axis_size(GROUP)
    moves = []
    for g in range(n_group):
        c, z, y = g // (2 * n_z), (g // 2) % n_z, g % 2
        moves.append((g, (z // 4) * 2 * n_z + (2 * (z % 4) + c) * 2 + y))
    kv_here = lax.ppermute(kv_part.astype(BF16), GROUP, moves)
    kv_all = to_all(kv_here, ("yh", "x", "zl", "yl")).reshape(n_dp, 2, HD, rows)
    key_t = jnp.moveaxis(kv_all[:, 0], 0, 1).reshape(HD, total)
    value_t = jnp.moveaxis(kv_all[:, 1], 0, 1).reshape(HD, total)

    key_pos = jnp.arange(total, dtype=jnp.int32)
    cos_k, sin_k = rope_tables(key_pos)
    cos_k, sin_k = cos_k.T, sin_k.T
    k1, k2 = key_t[: HD // 2].astype(F32), key_t[HD // 2 :].astype(F32)
    key_rot = jnp.concatenate(
        [k1 * cos_k - k2 * sin_k, k2 * cos_k + k1 * sin_k], axis=0
    ).astype(BF16)
    pos = block * rows + jnp.arange(rows, dtype=jnp.int32)
    cos_q, sin_q = rope_tables(pos)
    heads = w_query.shape[1] // HD
    q_rot = []
    for h in range(heads):
        q1 = query[:, h * HD : h * HD + HD // 2]
        q2 = query[:, h * HD + HD // 2 : (h + 1) * HD]
        q_rot.append(jnp.concatenate([q1 * cos_q - q2 * sin_q, q2 * cos_q + q1 * sin_q], axis=1))
    q_rot = jnp.concatenate(q_rot, axis=0).astype(BF16)
    scores = dot(q_rot, key_rot) * HD ** (-0.5)
    allowed = key_pos[None, :] <= jnp.tile(pos, heads)[:, None]
    scores = jnp.where(allowed, scores, -1e30)
    expo = jnp.exp(scores - jnp.max(scores, axis=-1, keepdims=True))
    probs = (expo / jnp.sum(expo, axis=-1, keepdims=True)).astype(BF16)
    attended = lax.dot_general(
        probs, value_t, (((1,), (1,)), ((), ())), preferred_element_type=F32
    ).astype(BF16)
    attended = jnp.concatenate([attended[h * rows : (h + 1) * rows] for h in range(heads)], axis=1)
    attended = attended.reshape(2, 2, quarter, heads * HD)
    attended = jnp.concatenate([pick(attended, y_lo, 1), pick(attended, 1 - y_lo, 1)], axis=0)
    attended = attended.reshape(rows, heads * HD)

    sent = lax.ppermute(out_terms(place, attended, w_out, True), "c", SWAP).astype(F32)
    terms = out_terms(place, attended, w_out, False)
    half = 2 * quarter
    far = (terms[:, half:] + sent[:, half:]).astype(BF16)
    far = lax.ppermute(far, "yl", SWAP).astype(F32)
    tiles = (terms[:, :half] + sent[:, :half] + far).astype(BF16)
    tiles = exchange(tiles.reshape(n_z, quarter, block_d), Z)
    at = ((x + z_hi) % NX, 0, (z_lo * 2 + y_lo) * quarter, 0)
    resid = [
        lax.dynamic_slice(t.reshape(NX, 2, rows, width), at, (1, 2, quarter, width))[0]
        for t in (own, far_rows)
    ]
    low = jnp.where(y_lo == 0, resid[0], resid[1])
    high = jnp.where(y_lo == 0, resid[1], resid[0])
    resid = jnp.concatenate([low[0], high[0], low[1], high[1]], axis=1)
    mid_part = (resid.astype(F32) + tiles.astype(F32).sum(axis=0)).astype(BF16)
    mid_own = move(mid_part, lambda c, yh, **_: {"c": yh, "yh": c})

    near = to_all(mid_own, Z).reshape(NX, half, block_d)
    near_c = lax.ppermute(near, "c", SWAP)
    far = lax.ppermute(near, "yl", SWAP)
    far_c = lax.ppermute(far, "c", SWAP)

    sent, keep, square = gate_up_terms(place, (near, far, near_c, far_c), gate_up_all)
    sent = lax.ppermute(sent, "yh", SWAP)
    hidden = hidden_units(keep, square, sent, dim)

    other = lax.ppermute(hidden, "yh", SWAP)
    sent = down_terms(place, hidden, other, down_all, True)
    sent = lax.ppermute(sent, "c", SWAP).astype(F32)
    terms = down_terms(place, hidden, other, down_all, False)
    far = (terms[:, half:] + sent[:, half:]).astype(BF16)
    far = lax.ppermute(far, "yl", SWAP).astype(F32)
    tiles = (terms[:, :half] + sent[:, :half] + far).astype(BF16)
    tiles = exchange(tiles.reshape(n_z, quarter, block_d), Z)
    done = (mid_own.astype(F32) + tiles.astype(F32).sum(axis=0)).astype(BF16)
    return move(done, lambda x, zh, **_: {"x": (x + zh) % NX, "zh": x})


def solution(mesh):
    fine = Mesh(mesh.devices.reshape(SIZES), EVERY)
    placed = (
        P(DP, GROUP),
        P(),
        P(None, GROUP),
        P(None, GROUP),
        P(GROUP, None),
        P(),
        P(DP, GROUP),
        P(DP, GROUP),
        P(GROUP, DP),
    )
    return jax.shard_map(layer, mesh=fine, in_specs=placed, out_specs=P(GROUP, DP), check_vma=False)
```

```python
import jax
import jax.numpy as jnp
from jax import lax
from jax.experimental import pallas as pl
from jax.experimental.pallas import tpu as pltpu
from jax.sharding import Mesh
from jax.sharding import PartitionSpec as P


HD = 128
EPS = 1e-05
THETA = 10000.0

F32 = jnp.float32
BF16 = jnp.bfloat16
DP = ("yh", "x")
Z = ("zh", "zl")
GROUP = ("c", "zh", "zl", "yl")
EVERY = ("c", "yh", "x", "zh", "zl", "yl")
SIZES = (2, 2, 4, 4, 2, 2)
SWAP = [(0, 1), (1, 0)]
NX = 4


def dot(a, b):
    return jnp.dot(a, b, preferred_element_type=F32)


def dot_t(a, b):
    return lax.dot_general(a, b, (((1,), (1,)), ((), ())), preferred_element_type=F32)


def from_z(array, r):
    return lax.ppermute(array, "zh", [(i, (i - r) % NX) for i in range(NX)])


def to_z(array, r):
    return from_z(array, -r)


def from_sq(array, s):
    return lax.ppermute(array, ("zl", "yl"), [(i, i ^ s) for i in range(4)])


def move(array, target):
    moves = []
    for n in range(256):
        at, rest = {}, n
        for name, size in zip(reversed(EVERY), reversed(SIZES)):
            at[name] = rest % size
            rest //= size
        goal, to = {**at, **target(**at)}, 0
        for name, size in zip(EVERY, SIZES):
            to = to * size + goal[name]
        moves.append((n, to))
    return lax.ppermute(array, EVERY, moves)


VMEM = pl.BlockSpec(memory_space=pltpu.VMEM)
SMEM = pl.BlockSpec(memory_space=pltpu.SMEM)
HBM = pl.BlockSpec(memory_space=pl.ANY)


def out_terms(place, attended, w_out, give):
    depth, block = w_out.shape[0], w_out.shape[1] // (2 * NX)
    heads = depth // HD
    rows = attended.shape[0] // heads
    quarter = rows // 4

    def body(place_ref, lhs_ref, w_hbm, out_ref, w, sem):
        half = 1 - place_ref[0] if give else place_ref[0]

        def copy(k):
            at = (half * NX + (place_ref[2] + place_ref[4] + k) % NX) * block
            return pltpu.make_async_copy(w_hbm.at[:, pl.ds(at, block)], w.at[k], sem.at[k])

        for k in range(NX):
            copy(k).start()
        lhs = []
        for s in range(4):
            at = (place_ref[1] ^ s) * quarter
            parts = [lhs_ref[pl.ds(h * rows + at, quarter)] for h in range(heads)]
            lhs.append(jnp.concatenate(parts, axis=1))
        lhs = jnp.concatenate(lhs, axis=0)
        for k in range(NX):
            copy(k).wait()
            out_ref[k] = dot(lhs, w[k]).astype(out_ref.dtype)

    return pl.pallas_call(
        body,
        out_shape=jax.ShapeDtypeStruct((NX, rows, block), BF16 if give else F32),
        in_specs=[SMEM, VMEM, HBM],
        out_specs=VMEM,
        scratch_shapes=[
            pltpu.VMEM((NX, depth, block), BF16),
            pltpu.SemaphoreType.DMA((NX,)),
        ],
        name="out_give" if give else "out_keep",
    )(place, attended, w_out)


def gate_up_terms(place, pieces, weights):
    n, part, depth = pieces[0].shape
    rows, cols, count = 4 * part, weights[0].shape[1], len(pieces)

    def body(place_ref, *refs):
        pieces, weights, refs = refs[:count], refs[count : count + n], refs[count + n :]
        give_ref, keep_ref, square_ref, w, acc, sq, sem = refs
        copies = [
            pltpu.make_async_copy(weights[k], w.at[k], sem.at[k]) for k in range(n)
        ]
        for copy in copies:
            copy.start()
        for k in range(n):
            r = (k + n - place_ref[4]) % n
            lhs = jnp.concatenate([p[r] for p in pieces], axis=0)
            wide = lhs.astype(F32)
            square = jnp.sum(wide * wide, axis=1, keepdims=True)
            copies[k].wait()
            out = dot(lhs, w[k])
            if k == 0:
                acc[...], sq[...] = out, jnp.broadcast_to(square, sq.shape)
            else:
                acc[...] += out
                sq[...] += square
        keep = pl.multiple_of((place_ref[3] ^ place_ref[0]) * rows, rows)
        give = pl.multiple_of(((1 - place_ref[3]) ^ place_ref[0]) * rows, rows)
        give_ref[:, :cols] = acc[pl.ds(give, rows)].astype(BF16)
        square = sq[pl.ds(give, rows)]
        top = square.astype(BF16)
        low = (square - top.astype(F32)).astype(BF16)
        lane = lax.broadcasted_iota(jnp.int32, square.shape, 1)
        give_ref[:, cols:] = jnp.where(lane == 0, top.astype(F32), low.astype(F32)).astype(BF16)
        keep_ref[...] = acc[pl.ds(keep, rows)]
        square_ref[...] = sq[pl.ds(keep, rows)]

    return pl.pallas_call(
        body,
        out_shape=[
            jax.ShapeDtypeStruct((rows, cols + 128), BF16),
            jax.ShapeDtypeStruct((rows, cols), F32),
            jax.ShapeDtypeStruct((rows, 128), F32),
        ],
        in_specs=[SMEM] + [VMEM] * count + [HBM] * n,
        out_specs=[VMEM] * 3,
        scratch_shapes=[
            pltpu.VMEM((n, depth, cols), BF16),
            pltpu.VMEM((2 * rows, cols), F32),
            pltpu.VMEM((2 * rows, 128), F32),
            pltpu.SemaphoreType.DMA((n,)),
        ],
        name="gate_up",
    )(place, *pieces, *weights)


def hidden_units(keep, square, sent, dim):
    rows, cols = keep.shape

    def body(keep_ref, square_ref, sent_ref, out_ref):
        extra = sent_ref[:, cols:].astype(F32)
        mean = (square_ref[:, :1] + extra[:, :1] + extra[:, 1:2]) / dim
        out = (keep_ref[...] + sent_ref[:, :cols].astype(F32)) * lax.rsqrt(mean + EPS)
        gate, up = out[:, : cols // 2], out[:, cols // 2 :]
        out_ref[...] = (gate / (1.0 + jnp.exp(-gate)) * up).astype(BF16)

    return pl.pallas_call(
        body,
        out_shape=jax.ShapeDtypeStruct((rows, cols // 2), BF16),
        in_specs=[VMEM] * 3,
        out_specs=VMEM,
        name="hidden",
    )(keep, square, sent)


def down_terms(place, hidden, other, weights, give):
    n, rows = len(weights), hidden.shape[0]
    depth, cols = weights[0].shape

    def body(place_ref, hidden_ref, other_ref, *refs):
        weights, out_ref, w, sem = refs[:n], refs[n], refs[n + 1], refs[n + 2]
        copies = [
            pltpu.make_async_copy(weights[k], w.at[k], sem.at[k]) for k in range(n)
        ]
        for copy in copies:
            copy.start()
        same = place_ref[0] == place_ref[3]
        own = jnp.logical_not(same) if give else same
        lhs = jnp.where(own, hidden_ref[...], other_ref[...])
        for k in range(n):
            copies[k].wait()
            out_ref[(k + n - place_ref[4]) % n] = dot(lhs, w[k]).astype(out_ref.dtype)

    return pl.pallas_call(
        body,
        out_shape=jax.ShapeDtypeStruct((n, rows, cols), BF16 if give else F32),
        in_specs=[SMEM, VMEM, VMEM] + [HBM] * n,
        out_specs=VMEM,
        scratch_shapes=[pltpu.VMEM((n, depth, cols), BF16), pltpu.SemaphoreType.DMA((n,))],
        name="down_give" if give else "down_keep",
    )(place, hidden, other, *weights)


def rope_tables(positions):
    half = HD // 2
    frequency = THETA ** (-jnp.arange(half, dtype=F32) * 2.0 / HD)
    angles = positions.astype(F32)[:, None] * frequency[None, :]
    return jnp.cos(angles), jnp.sin(angles)


def pick(array, index, axis=0):
    return lax.dynamic_index_in_dim(array, index, axis, keepdims=False)


def from_x(array, r):
    return lax.ppermute(array, "x", [(i, (i - r) % NX) for i in range(NX)])


def project(place, pieces, gains, w_query, w_keyval, sums):
    arrays = [piece for piece, _, _ in pieces]
    n_z, rows, width = arrays[0].shape
    n_q, n_kv = w_query.shape[1], w_keyval.shape[0]
    steps = n_z * len(arrays)
    last = sums is not None

    def body(place_ref, gain_ref, wq_hbm, wkv_hbm, *refs):
        refs, rest = refs[: len(arrays)], refs[len(arrays) :]
        before, rest = (rest[:3], rest[3:]) if last else (None, rest)
        q_ref, kv_ref, sq_ref, wq, wkv, sem_q, sem_kv = rest

        def at(i):
            _, s, rc = pieces[i // n_z]
            zh = (place_ref[4] + i % n_z) % n_z
            return ((place_ref[0] ^ rc) * n_z + zh) * 4 + (place_ref[1] ^ s)

        def copies(i):
            g = at(i) * width
            return (
                pltpu.make_async_copy(wq_hbm.at[pl.ds(g, width)], wq.at[i], sem_q.at[i]),
                pltpu.make_async_copy(wkv_hbm.at[:, pl.ds(g, width)], wkv.at[i], sem_kv.at[i]),
            )

        for i in range(steps):
            for copy in copies(i):
                copy.start()
        for i in range(steps):
            piece = refs[i // n_z][i % n_z].astype(F32)
            lhs = (piece * gain_ref[at(i)]).astype(BF16)
            part = piece * piece
            for copy in copies(i):
                copy.wait()
            q, kv = dot(lhs, wq[i]), dot_t(wkv[i], lhs)
            if i == 0 and not last:
                sq_ref[...], q_ref[...], kv_ref[...] = part, q, kv
            elif i == 0:
                sq_ref[...] = before[2][...] + part
                q_ref[...] = before[0][...] + q
                kv_ref[...] = before[1][...] + kv
            else:
                sq_ref[...] += part
                q_ref[...] += q
                kv_ref[...] += kv
        if last:
            mean = jnp.sum(sq_ref[...], axis=1, keepdims=True) / (32 * width)
            factor = lax.rsqrt(mean + EPS)
            q_ref[...] = q_ref[...] * factor
            across = jnp.broadcast_to(factor, (rows, rows)).T[:1]
            kv_ref[...] = kv_ref[...] * across

    shapes = [(rows, n_q), (n_kv, rows), (rows, width)]
    return pl.pallas_call(
        body,
        out_shape=[jax.ShapeDtypeStruct(shape, F32) for shape in shapes],
        in_specs=[SMEM, VMEM, HBM, HBM] + [VMEM] * (len(arrays) + (3 if last else 0)),
        out_specs=[VMEM] * 3,
        scratch_shapes=[
            pltpu.VMEM((steps, width, n_q), BF16),
            pltpu.VMEM((steps, n_kv, width), BF16),
            pltpu.SemaphoreType.DMA((steps,)),
            pltpu.SemaphoreType.DMA((steps,)),
        ],
        name="project_last" if last else "project_first",
    )(place, gains, w_query, w_keyval, *arrays, *(sums or ()))


def summed(terms, sent):
    quarter = terms.shape[1] // 4

    def both(s):
        rows = slice(s * quarter, (s + 1) * quarter)
        return terms[:, rows] + sent[:, rows].astype(F32)

    got = [from_sq(both(s).astype(BF16), s) for s in (1, 2, 3)]
    mine = both(0) + sum(t.astype(F32) for t in got)
    got = [to_z(mine[r].astype(BF16), r) for r in (2, 1, 3)]
    return mine[0] + sum(t.astype(F32) for t in got)


def gathered(piece):
    got = {r: from_z(piece, r) for r in (2, 1, 3)}
    near = jnp.stack([piece, got[1], got[2], got[3]], axis=0)
    ours = [near] + [from_sq(near, s) for s in (1, 2, 3)]
    theirs = [lax.ppermute(t, "c", SWAP) for t in ours]
    return ours, theirs


def layer(tokens_in, gain_attn, w_query, w_keyval, w_out, gain_mlp, w_gate, w_up, w_down):
    core, y_hi, x = lax.axis_index("c"), lax.axis_index("yh"), lax.axis_index("x")
    z_hi, z_lo, y_lo = lax.axis_index("zh"), lax.axis_index("zl"), lax.axis_index("yl")
    block, spot = lax.axis_index(DP), z_lo * 2 + y_lo
    rows, width = tokens_in.shape
    n_dp, n_z = lax.axis_size(DP), lax.axis_size(Z)
    dim = w_query.shape[0]
    block_d = dim // 8
    total = rows * n_dp
    quarter = rows // 4

    gain_cols = lax.dynamic_slice_in_dim(gain_mlp, block * block_d, block_d, 0)
    gate_up_w = jnp.concatenate([w_gate, w_up], axis=1).astype(F32)
    gate_up_w = (gate_up_w * gain_cols.astype(F32)[:, None]).astype(BF16)

    gate_up_next, gate_up_last = from_x(gate_up_w, 1), from_x(gate_up_w, 3)
    gate_up_all = [gate_up_w, gate_up_next, from_x(gate_up_w, 2), gate_up_last]
    down_all = [w_down] + [from_x(w_down, r) for r in range(1, NX)]

    ours, theirs = gathered(tokens_in)
    place = jnp.stack([core, spot, x, y_hi, z_hi]).astype(jnp.int32)
    gains = gain_attn.astype(F32).reshape(4 * n_z, 1, width)
    pieces = [(t, s, rc) for rc, side in ((0, ours), (1, theirs)) for s, t in enumerate(side)]
    early = [p for p in pieces if p[1] == 0]
    late = [p for p in pieces if p[1] != 0]
    w_kv = w_keyval.T
    sums = project(place, early, gains, w_query, w_kv, None)
    query, kv_part, _ = project(place, late, gains, w_query, w_kv, sums)

    n_group = lax.axis_size(GROUP)
    moves = []
    for g in range(n_group):
        c, z, y = g // (2 * n_z), (g // 2) % n_z, g % 2
        moves.append((g, (z // 4) * 2 * n_z + (2 * (z % 4) + c) * 2 + y))
    kv_here = lax.ppermute(kv_part.astype(BF16), GROUP, moves)
    parts = jnp.stack([kv_here] + [from_sq(kv_here, t) for t in (1, 2, 3)], axis=0)
    parts = jnp.concatenate([pick(parts, j ^ spot) for j in range(4)], axis=0)
    parts = jnp.stack([parts, lax.ppermute(parts, "yh", SWAP)], axis=0)
    parts = jnp.stack([parts] + [from_x(parts, r) for r in range(1, NX)], axis=0)
    parts = parts.reshape(n_dp, 2, HD, rows)
    key_t = jnp.moveaxis(parts[:, 0], 0, 1).reshape(HD, total)
    value_t = jnp.moveaxis(parts[:, 1], 0, 1).reshape(HD, total)

    blocks = jnp.stack(
        [(y_hi ^ ry) * NX + (x + r) % NX for r in range(NX) for ry in range(2)]
    )
    key_pos = blocks.astype(jnp.int32)[:, None] * rows + jnp.arange(rows, dtype=jnp.int32)
    key_pos = key_pos.reshape(total)
    cos_k, sin_k = rope_tables(key_pos)
    cos_k, sin_k = cos_k.T, sin_k.T
    k1, k2 = key_t[: HD // 2].astype(F32), key_t[HD // 2 :].astype(F32)
    key_rot = jnp.concatenate(
        [k1 * cos_k - k2 * sin_k, k2 * cos_k + k1 * sin_k], axis=0
    ).astype(BF16)
    pos = block * rows + jnp.arange(rows, dtype=jnp.int32)
    cos_q, sin_q = rope_tables(pos)
    heads = w_query.shape[1] // HD
    q_rot = []
    for h in range(heads):
        q1 = query[:, h * HD : h * HD + HD // 2]
        q2 = query[:, h * HD + HD // 2 : (h + 1) * HD]
        q_rot.append(jnp.concatenate([q1 * cos_q - q2 * sin_q, q2 * cos_q + q1 * sin_q], axis=1))
    q_rot = jnp.concatenate(q_rot, axis=0).astype(BF16)
    scores = dot(q_rot, key_rot) * HD ** (-0.5)
    allowed = key_pos[None, :] <= jnp.tile(pos, heads)[:, None]
    scores = jnp.where(allowed, scores, -1e30)
    expo = jnp.exp(scores - jnp.max(scores, axis=-1, keepdims=True))
    probs = (expo / jnp.sum(expo, axis=-1, keepdims=True)).astype(BF16)
    attended = lax.dot_general(
        probs, value_t, (((1,), (1,)), ((), ())), preferred_element_type=F32
    ).astype(BF16)
    sent = lax.ppermute(out_terms(place, attended, w_out, True), "c", SWAP)
    terms = out_terms(place, attended, w_out, False)
    resid = [
        lax.dynamic_slice(t, (x, spot * quarter, 0), (1, quarter, width))[0] for t in ours
    ]
    resid = jnp.stack(resid, axis=0)
    resid = jnp.concatenate([pick(resid, j ^ spot) for j in range(4)], axis=1)
    mid_part = (resid.astype(F32) + summed(terms, sent)).astype(BF16)
    mid_own = move(mid_part, lambda c, yh, **_: {"c": yh, "yh": c})

    ours, theirs = gathered(mid_own)

    sent, keep, square = gate_up_terms(place, ours + theirs, gate_up_all)
    sent = lax.ppermute(sent, "yh", SWAP)
    hidden = hidden_units(keep, square, sent, dim)

    other = lax.ppermute(hidden, "yh", SWAP)
    sent = down_terms(place, hidden, other, down_all, True)
    sent = lax.ppermute(sent, "c", SWAP)
    terms = down_terms(place, hidden, other, down_all, False)
    done = (mid_own.astype(F32) + summed(terms, sent)).astype(BF16)
    return move(done, lambda x, zh, **_: {"x": (x + zh) % NX, "zh": x})


def solution(mesh):
    fine = Mesh(mesh.devices.reshape(SIZES), EVERY)
    placed = (
        P(DP, GROUP),
        P(),
        P(None, GROUP),
        P(None, GROUP),
        P(GROUP, None),
        P(),
        P(DP, GROUP),
        P(DP, GROUP),
        P(GROUP, DP),
    )
    return jax.shard_map(layer, mesh=fine, in_specs=placed, out_specs=P(GROUP, DP), check_vma=False)
```

```python
import jax
import jax.numpy as jnp
from jax import lax
from jax.experimental import pallas as pl
from jax.experimental.pallas import tpu as pltpu
from jax.sharding import Mesh
from jax.sharding import PartitionSpec as P


HD = 128
EPS = 1e-05
THETA = 10000.0

F32 = jnp.float32
BF16 = jnp.bfloat16
DP = ("yh", "x")
Z = ("zh", "zl")
GROUP = ("c", "zh", "zl", "yl")
EVERY = ("c", "yh", "x", "zh", "zl", "yl")
SIZES = (2, 2, 4, 4, 2, 2)
SWAP = [(0, 1), (1, 0)]
NX = 4


def dot(a, b):
    return jnp.dot(a, b, preferred_element_type=F32)


def dot_t(a, b):
    return lax.dot_general(a, b, (((1,), (1,)), ((), ())), preferred_element_type=F32)


def to_all(array, axis):
    length = lax.axis_size(axis)
    return exchange(jnp.broadcast_to(array[None], (length, *array.shape)), axis)


def exchange(tiles, axis):
    return lax.all_to_all(tiles, axis, 0, 0, tiled=True)


def from_sq(array, s):
    return lax.ppermute(array, ("zl", "yl"), [(i, i ^ s) for i in range(4)])


def move(array, target):
    moves = []
    for n in range(256):
        at, rest = {}, n
        for name, size in zip(reversed(EVERY), reversed(SIZES)):
            at[name] = rest % size
            rest //= size
        goal, to = {**at, **target(**at)}, 0
        for name, size in zip(EVERY, SIZES):
            to = to * size + goal[name]
        moves.append((n, to))
    return lax.ppermute(array, EVERY, moves)


VMEM = pl.BlockSpec(memory_space=pltpu.VMEM)
SMEM = pl.BlockSpec(memory_space=pltpu.SMEM)
HBM = pl.BlockSpec(memory_space=pl.ANY)


def in_vmem(*arrays):
    return [pltpu.with_memory_space_constraint(t, pltpu.VMEM) for t in arrays]


def out_terms(place, attended, w_out, give):
    depth, block = w_out.shape[0], w_out.shape[1] // (2 * NX)
    heads = depth // HD
    rows = attended.shape[0] // heads
    quarter = rows // 4

    def body(place_ref, lhs_ref, w_hbm, out_ref, w, sem):
        half = 1 - place_ref[0] if give else place_ref[0]

        def copy(k):
            at = (half * NX + (place_ref[2] + k) % NX) * block
            return pltpu.make_async_copy(w_hbm.at[:, pl.ds(at, block)], w.at[k], sem.at[k])

        for k in range(NX):
            copy(k).start()
        lhs = []
        for s in range(4):
            at = (place_ref[1] ^ s) * quarter
            parts = [lhs_ref[pl.ds(h * rows + at, quarter)] for h in range(heads)]
            lhs.append(jnp.concatenate(parts, axis=1))
        lhs = jnp.concatenate(lhs, axis=0)
        for k in range(NX):
            copy(k).wait()
            out_ref[k] = dot(lhs, w[k]).astype(out_ref.dtype)

    return pl.pallas_call(
        body,
        out_shape=pltpu.VMEM((NX, rows, block), BF16 if give else F32),
        in_specs=[SMEM, VMEM, HBM],
        out_specs=VMEM,
        scratch_shapes=[
            pltpu.VMEM((NX, depth, block), BF16),
            pltpu.SemaphoreType.DMA((NX,)),
        ],
        name="out_give" if give else "out_keep",
    )(place, *in_vmem(attended), w_out)


def gate_up_terms(place, pieces, weights):
    n, part, depth = pieces[0].shape
    rows, cols, count = 4 * part, weights[0].shape[1], len(pieces)

    def body(place_ref, *refs):
        pieces, weights, refs = refs[:count], refs[count : count + n], refs[count + n :]
        give_ref, keep_ref, square_ref, w, acc, sq, sem = refs
        copies = [
            pltpu.make_async_copy(weights[k], w.at[k], sem.at[k]) for k in range(n)
        ]
        for copy in copies:
            copy.start()
        for k in range(n):
            lhs = jnp.concatenate([p[k] for p in pieces], axis=0)
            wide = lhs.astype(F32)
            square = jnp.sum(wide * wide, axis=1, keepdims=True)
            copies[k].wait()
            out = dot(lhs, w[k])
            if k == 0:
                acc[...], sq[...] = out, jnp.broadcast_to(square, sq.shape)
            else:
                acc[...] += out
                sq[...] += square
        keep = pl.multiple_of((place_ref[3] ^ place_ref[0]) * rows, rows)
        give = pl.multiple_of(((1 - place_ref[3]) ^ place_ref[0]) * rows, rows)
        give_ref[:, :cols] = acc[pl.ds(give, rows)].astype(BF16)
        square = sq[pl.ds(give, rows)]
        top = square.astype(BF16)
        low = (square - top.astype(F32)).astype(BF16)
        lane = lax.broadcasted_iota(jnp.int32, square.shape, 1)
        give_ref[:, cols:] = jnp.where(lane == 0, top.astype(F32), low.astype(F32)).astype(BF16)
        keep_ref[...] = acc[pl.ds(keep, rows)]
        square_ref[...] = sq[pl.ds(keep, rows)]

    return pl.pallas_call(
        body,
        out_shape=[
            pltpu.VMEM((rows, cols + 128), BF16),
            pltpu.VMEM((rows, cols), F32),
            pltpu.VMEM((rows, 128), F32),
        ],
        in_specs=[SMEM] + [VMEM] * count + [HBM] * n,
        out_specs=[VMEM] * 3,
        scratch_shapes=[
            pltpu.VMEM((n, depth, cols), BF16),
            pltpu.VMEM((2 * rows, cols), F32),
            pltpu.VMEM((2 * rows, 128), F32),
            pltpu.SemaphoreType.DMA((n,)),
        ],
        name="gate_up",
    )(place, *in_vmem(*pieces), *weights)


def hidden_units(keep, square, sent, dim):
    rows, cols = keep.shape

    def body(keep_ref, square_ref, sent_ref, out_ref):
        extra = sent_ref[:, cols:].astype(F32)
        mean = (square_ref[:, :1] + extra[:, :1] + extra[:, 1:2]) / dim
        out = (keep_ref[...] + sent_ref[:, :cols].astype(F32)) * lax.rsqrt(mean + EPS)
        gate, up = out[:, : cols // 2], out[:, cols // 2 :]
        out_ref[...] = (gate / (1.0 + jnp.exp(-gate)) * up).astype(BF16)

    return pl.pallas_call(
        body,
        out_shape=pltpu.VMEM((rows, cols // 2), BF16),
        in_specs=[VMEM] * 3,
        out_specs=VMEM,
        name="hidden",
    )(*in_vmem(keep, square, sent))


def down_terms(place, hidden, other, weights, give):
    n, rows = len(weights), hidden.shape[0]
    depth, cols = weights[0].shape

    def body(place_ref, hidden_ref, other_ref, *refs):
        weights, out_ref, w, sem = refs[:n], refs[n], refs[n + 1], refs[n + 2]
        copies = [
            pltpu.make_async_copy(weights[k], w.at[k], sem.at[k]) for k in range(n)
        ]
        for copy in copies:
            copy.start()
        same = place_ref[0] == place_ref[3]
        own = jnp.logical_not(same) if give else same
        lhs = jnp.where(own, hidden_ref[...], other_ref[...])
        for k in range(n):
            copies[k].wait()
            out_ref[k] = dot(lhs, w[k]).astype(out_ref.dtype)

    return pl.pallas_call(
        body,
        out_shape=pltpu.VMEM((n, rows, cols), BF16 if give else F32),
        in_specs=[SMEM, VMEM, VMEM] + [HBM] * n,
        out_specs=VMEM,
        scratch_shapes=[pltpu.VMEM((n, depth, cols), BF16), pltpu.SemaphoreType.DMA((n,))],
        name="down_give" if give else "down_keep",
    )(place, *in_vmem(hidden, other), *weights)


def rope_tables(positions):
    half = HD // 2
    frequency = THETA ** (-jnp.arange(half, dtype=F32) * 2.0 / HD)
    angles = positions.astype(F32)[:, None] * frequency[None, :]
    return jnp.cos(angles), jnp.sin(angles)


def pick(array, index, axis=0):
    return lax.dynamic_index_in_dim(array, index, axis, keepdims=False)


def from_x(array, r):
    return lax.ppermute(array, "x", [(i, (i - r) % NX) for i in range(NX)])


def project(place, pieces, gains, w_query, w_keyval, sums):
    arrays = [piece for piece, _, _ in pieces]
    n_z, rows, width = arrays[0].shape
    n_q, n_kv = w_query.shape[1], w_keyval.shape[0]
    steps = n_z * len(arrays)
    last = sums is not None

    def body(place_ref, gain_ref, wq_hbm, wkv_hbm, *refs):
        refs, rest = refs[: len(arrays)], refs[len(arrays) :]
        before, rest = (rest[:3], rest[3:]) if last else (None, rest)
        q_ref, kv_ref, sq_ref, wq, wkv, sem_q, sem_kv = rest

        def at(i):
            _, s, rc = pieces[i // n_z]
            return ((place_ref[0] ^ rc) * n_z + i % n_z) * 4 + (place_ref[1] ^ s)

        def copies(i):
            g = at(i) * width
            return (
                pltpu.make_async_copy(wq_hbm.at[pl.ds(g, width)], wq.at[i], sem_q.at[i]),
                pltpu.make_async_copy(wkv_hbm.at[:, pl.ds(g, width)], wkv.at[i], sem_kv.at[i]),
            )

        for i in range(steps):
            for copy in copies(i):
                copy.start()
        if last:
            for ref, old in zip((q_ref, kv_ref, sq_ref), before):
                ref[...] = old[...]
        else:
            for ref in (q_ref, kv_ref, sq_ref):
                ref[...] = jnp.zeros(ref.shape, F32)
        for p, ref in enumerate(refs):
            q, kv = q_ref[...], kv_ref[...]
            for r in range(n_z):
                i = p * n_z + r
                piece = ref[r].astype(F32)
                lhs = (piece * gain_ref[at(i)]).astype(BF16)
                sq_ref[...] += piece * piece
                for copy in copies(i):
                    copy.wait()
                q, kv = q + dot(lhs, wq[i]), kv + dot_t(wkv[i], lhs)
            q_ref[...], kv_ref[...] = q, kv
        if last:
            mean = jnp.sum(sq_ref[...], axis=1, keepdims=True) / (32 * width)
            factor = lax.rsqrt(mean + EPS)
            q_ref[...] = q_ref[...] * factor
            across = jnp.broadcast_to(factor, (rows, rows)).T[:1]
            kv_ref[...] = kv_ref[...] * across

    shapes = [(rows, n_q), (n_kv, rows), (rows, width)]
    return pl.pallas_call(
        body,
        out_shape=[pltpu.VMEM(shape, F32) for shape in shapes],
        in_specs=[SMEM, VMEM, HBM, HBM] + [VMEM] * (len(arrays) + (3 if last else 0)),
        out_specs=[VMEM] * 3,
        scratch_shapes=[
            pltpu.VMEM((steps, width, n_q), BF16),
            pltpu.VMEM((steps, n_kv, width), BF16),
            pltpu.SemaphoreType.DMA((steps,)),
            pltpu.SemaphoreType.DMA((steps,)),
        ],
        name="project_last" if last else "project_first",
    )(place, *in_vmem(gains), w_query, w_keyval, *in_vmem(*arrays, *(sums or ())))


def summed(terms, sent):
    quarter = terms.shape[1] // 4

    def both(s):
        rows = slice(s * quarter, (s + 1) * quarter)
        return terms[:, rows] + sent[:, rows].astype(F32)

    got = [from_sq(both(s).astype(BF16), s) for s in (1, 2, 3)]
    mine = both(0) + sum(t.astype(F32) for t in got)
    tiles = exchange(mine.astype(BF16), "zh")
    return tiles.astype(F32).sum(axis=0)


def gathered(piece):
    near = to_all(piece, "zh")
    ours = [near] + [from_sq(near, s) for s in (1, 2, 3)]
    theirs = [lax.ppermute(t, "c", SWAP) for t in ours]
    return ours, theirs


def layer(tokens_in, gain_attn, w_query, w_keyval, w_out, gain_mlp, w_gate, w_up, w_down):
    core, y_hi, x = lax.axis_index("c"), lax.axis_index("yh"), lax.axis_index("x")
    z_hi, z_lo, y_lo = lax.axis_index("zh"), lax.axis_index("zl"), lax.axis_index("yl")
    block, spot = lax.axis_index(DP), z_lo * 2 + y_lo
    rows, width = tokens_in.shape
    n_dp, n_z = lax.axis_size(DP), lax.axis_size(Z)
    dim = w_query.shape[0]
    block_d = dim // 8
    total = rows * n_dp
    quarter = rows // 4

    down_next, down_last = from_x(w_down, 1), from_x(w_down, 3)
    gain_cols = lax.dynamic_slice_in_dim(gain_mlp, block * block_d, block_d, 0)
    gate_up_w = jnp.concatenate([w_gate, w_up], axis=1).astype(F32)
    gate_up_w = (gate_up_w * gain_cols.astype(F32)[:, None]).astype(BF16)
    gate_up_all = [gate_up_w] + [from_x(gate_up_w, r) for r in range(1, NX)]
    down_all = [w_down, down_next, from_x(w_down, 2), down_last]

    ours, theirs = gathered(tokens_in)
    place = jnp.stack([core, spot, x, y_hi]).astype(jnp.int32)
    gains = gain_attn.astype(F32).reshape(4 * n_z, 1, width)
    pieces = [(t, s, rc) for rc, side in ((0, ours), (1, theirs)) for s, t in enumerate(side)]
    early = [p for p in pieces if p[1] == 0]
    late = [p for p in pieces if p[1] != 0]
    w_kv = w_keyval.T
    sums = project(place, early, gains, w_query, w_kv, None)
    query, kv_part, _ = project(place, late, gains, w_query, w_kv, sums)

    kv_here = kv_part.astype(BF16)
    parts = []
    for t in range(4):
        parts.append(
            move(
                kv_here,
                lambda c, zh, zl, yl, t=t, **_: {
                    "c": zh // 2,
                    "zh": (zh % 2) * 2 + zl,
                    "zl": c ^ (t >> 1),
                    "yl": yl ^ (t & 1),
                },
            )
        )
    parts = jnp.stack(parts, axis=0)
    parts = jnp.concatenate([pick(parts, j ^ spot) for j in range(4)], axis=0)
    parts = jnp.stack([parts, lax.ppermute(parts, "yh", SWAP)], axis=0)
    parts = jnp.stack([parts] + [from_x(parts, r) for r in range(1, NX)], axis=0)
    parts = parts.reshape(n_dp, 2, HD, rows)
    key_t = jnp.moveaxis(parts[:, 0], 0, 1).reshape(HD, total)
    value_t = jnp.moveaxis(parts[:, 1], 0, 1).reshape(HD, total)

    blocks = jnp.stack(
        [(y_hi ^ ry) * NX + (x + r) % NX for r in range(NX) for ry in range(2)]
    )
    key_pos = blocks.astype(jnp.int32)[:, None] * rows + jnp.arange(rows, dtype=jnp.int32)
    key_pos = key_pos.reshape(total)
    cos_k, sin_k = rope_tables(key_pos)
    cos_k, sin_k = cos_k.T, sin_k.T
    k1, k2 = key_t[: HD // 2].astype(F32), key_t[HD // 2 :].astype(F32)
    key_rot = jnp.concatenate(
        [k1 * cos_k - k2 * sin_k, k2 * cos_k + k1 * sin_k], axis=0
    ).astype(BF16)
    pos = block * rows + jnp.arange(rows, dtype=jnp.int32)
    cos_q, sin_q = rope_tables(pos)
    heads = w_query.shape[1] // HD
    q_rot = []
    for h in range(heads):
        q1 = query[:, h * HD : h * HD + HD // 2]
        q2 = query[:, h * HD + HD // 2 : (h + 1) * HD]
        q_rot.append(jnp.concatenate([q1 * cos_q - q2 * sin_q, q2 * cos_q + q1 * sin_q], axis=1))
    q_rot = jnp.concatenate(q_rot, axis=0).astype(BF16)
    scores = dot(q_rot, key_rot) * HD ** (-0.5)
    allowed = key_pos[None, :] <= jnp.tile(pos, heads)[:, None]
    scores = jnp.where(allowed, scores, -1e30)
    expo = jnp.exp(scores - jnp.max(scores, axis=-1, keepdims=True))
    probs = (expo / jnp.sum(expo, axis=-1, keepdims=True)).astype(BF16)
    attended = lax.dot_general(
        probs, value_t, (((1,), (1,)), ((), ())), preferred_element_type=F32
    ).astype(BF16)
    sent = lax.ppermute(out_terms(place, attended, w_out, True), "c", SWAP)
    terms = out_terms(place, attended, w_out, False)
    resid = [
        lax.dynamic_slice(t, ((x + z_hi) % NX, spot * quarter, 0), (1, quarter, width))[0]
        for t in ours
    ]
    resid = jnp.stack(resid, axis=0)
    resid = jnp.concatenate([pick(resid, j ^ spot) for j in range(4)], axis=1)
    mid_part = (resid.astype(F32) + summed(terms, sent)).astype(BF16)
    mid_own = move(mid_part, lambda c, yh, **_: {"c": yh, "yh": c})

    ours, theirs = gathered(mid_own)

    sent, keep, square = gate_up_terms(place, ours + theirs, gate_up_all)
    sent = lax.ppermute(sent, "yh", SWAP)
    hidden = hidden_units(keep, square, sent, dim)

    other = lax.ppermute(hidden, "yh", SWAP)
    sent = down_terms(place, hidden, other, down_all, True)
    sent = lax.ppermute(sent, "c", SWAP)
    terms = down_terms(place, hidden, other, down_all, False)
    done = (mid_own.astype(F32) + summed(terms, sent)).astype(BF16)
    return move(done, lambda x, zh, **_: {"x": (x + zh) % NX, "zh": x})


def solution(mesh):
    fine = Mesh(mesh.devices.reshape(SIZES), EVERY)
    placed = (
        P(DP, GROUP),
        P(),
        P(None, GROUP),
        P(None, GROUP),
        P(GROUP, None),
        P(),
        P(DP, GROUP),
        P(DP, GROUP),
        P(GROUP, DP),
    )
    return jax.shard_map(layer, mesh=fine, in_specs=placed, out_specs=P(GROUP, DP), check_vma=False)
```

```python
import jax
import jax.numpy as jnp
from jax import lax
from jax.experimental import pallas as pl
from jax.experimental.pallas import tpu as pltpu
from jax.sharding import Mesh
from jax.sharding import PartitionSpec as P


HD = 128
EPS = 1e-05
THETA = 10000.0

F32 = jnp.float32
BF16 = jnp.bfloat16
DP = ("yh", "x")
Z = ("zh", "zl")
GROUP = ("c", "zh", "zl", "yl")
EVERY = ("c", "yh", "x", "zh", "zl", "yl")
SIZES = (2, 2, 4, 4, 2, 2)
SWAP = [(0, 1), (1, 0)]
NX = 4


def dot(a, b):
    return jnp.dot(a, b, preferred_element_type=F32)


def dot_t(a, b):
    return lax.dot_general(a, b, (((1,), (1,)), ((), ())), preferred_element_type=F32)


def to_all(array, axis):
    length = lax.axis_size(axis)
    return exchange(jnp.broadcast_to(array[None], (length, *array.shape)), axis)


def exchange(tiles, axis):
    return lax.all_to_all(tiles, axis, 0, 0, tiled=True)


def from_sq(array, s):
    return lax.ppermute(array, ("zl", "yl"), [(i, i ^ s) for i in range(4)])


def move(array, target):
    moves = []
    for n in range(256):
        at, rest = {}, n
        for name, size in zip(reversed(EVERY), reversed(SIZES)):
            at[name] = rest % size
            rest //= size
        goal, to = {**at, **target(**at)}, 0
        for name, size in zip(EVERY, SIZES):
            to = to * size + goal[name]
        moves.append((n, to))
    return lax.ppermute(array, EVERY, moves)


VMEM = pl.BlockSpec(memory_space=pltpu.VMEM)
SMEM = pl.BlockSpec(memory_space=pltpu.SMEM)
HBM = pl.BlockSpec(memory_space=pl.ANY)


def in_vmem(*arrays):
    return [pltpu.with_memory_space_constraint(t, pltpu.VMEM) for t in arrays]


def out_terms(place, attended, w_out, give):
    depth, block = w_out.shape[0], w_out.shape[1] // (2 * NX)
    heads = depth // HD
    rows = attended.shape[0] // heads
    quarter = rows // 4

    def body(place_ref, lhs_ref, w_hbm, out_ref, w, sem):
        half = 1 - place_ref[0] if give else place_ref[0]

        def copy(k):
            at = (half * NX + (place_ref[2] + k) % NX) * block
            return pltpu.make_async_copy(w_hbm.at[:, pl.ds(at, block)], w.at[k], sem.at[k])

        for k in range(NX):
            copy(k).start()
        lhs = []
        for s in range(4):
            at = (place_ref[1] ^ s) * quarter
            parts = [lhs_ref[pl.ds(h * rows + at, quarter)] for h in range(heads)]
            lhs.append(jnp.concatenate(parts, axis=1))
        lhs = jnp.concatenate(lhs, axis=0)
        for k in range(NX):
            copy(k).wait()
            out_ref[k] = dot(lhs, w[k]).astype(out_ref.dtype)

    return pl.pallas_call(
        body,
        out_shape=pltpu.VMEM((NX, rows, block), BF16 if give else F32),
        in_specs=[SMEM, VMEM, HBM],
        out_specs=VMEM,
        scratch_shapes=[
            pltpu.VMEM((NX, depth, block), BF16),
            pltpu.SemaphoreType.DMA((NX,)),
        ],
        name="out_give" if give else "out_keep",
    )(place, *in_vmem(attended), w_out)


def gate_up_terms(place, gains, pieces, weights):
    n, part, depth = pieces[0].shape
    rows, cols, count = 4 * part, weights[0].shape[1], len(pieces)

    def body(place_ref, gain_ref, *refs):
        pieces, weights, refs = refs[:count], refs[count : count + n], refs[count + n :]
        give_ref, keep_ref, square_ref, w, acc, sq, sem = refs
        copies = [
            pltpu.make_async_copy(weights[k], w.at[k], sem.at[k]) for k in range(n)
        ]
        for copy in copies:
            copy.start()
        for k in range(n):
            lhs = jnp.concatenate([p[k] for p in pieces], axis=0)
            wide = lhs.astype(F32)
            square = jnp.sum(wide * wide, axis=1, keepdims=True)
            copies[k].wait()
            gain = gain_ref[place_ref[3] * n + (place_ref[2] + k) % n]
            out = dot((wide * gain).astype(BF16), w[k])
            if k == 0:
                acc[...], sq[...] = out, jnp.broadcast_to(square, sq.shape)
            else:
                acc[...] += out
                sq[...] += square
        keep = pl.multiple_of((place_ref[3] ^ place_ref[0]) * rows, rows)
        give = pl.multiple_of(((1 - place_ref[3]) ^ place_ref[0]) * rows, rows)
        give_ref[:, :cols] = acc[pl.ds(give, rows)].astype(BF16)
        square = sq[pl.ds(give, rows)]
        top = square.astype(BF16)
        low = (square - top.astype(F32)).astype(BF16)
        lane = lax.broadcasted_iota(jnp.int32, square.shape, 1)
        give_ref[:, cols:] = jnp.where(lane == 0, top.astype(F32), low.astype(F32)).astype(BF16)
        keep_ref[...] = acc[pl.ds(keep, rows)]
        square_ref[...] = sq[pl.ds(keep, rows)]

    return pl.pallas_call(
        body,
        out_shape=[
            pltpu.VMEM((rows, cols + 128), BF16),
            jax.ShapeDtypeStruct((rows, cols), F32),
            jax.ShapeDtypeStruct((rows, 128), F32),
        ],
        in_specs=[SMEM, VMEM] + [VMEM] * count + [HBM] * n,
        out_specs=[VMEM] * 3,
        scratch_shapes=[
            pltpu.VMEM((n, depth, cols), BF16),
            pltpu.VMEM((2 * rows, cols), F32),
            pltpu.VMEM((2 * rows, 128), F32),
            pltpu.SemaphoreType.DMA((n,)),
        ],
        name="gate_up",
    )(place, gains, *in_vmem(*pieces), *weights)


def hidden_units(keep, square, sent, dim):
    rows, cols = keep.shape

    def body(keep_ref, square_ref, sent_ref, out_ref):
        extra = sent_ref[:, cols:].astype(F32)
        mean = (square_ref[:, :1] + extra[:, :1] + extra[:, 1:2]) / dim
        out = (keep_ref[...] + sent_ref[:, :cols].astype(F32)) * lax.rsqrt(mean + EPS)
        gate, up = out[:, : cols // 2], out[:, cols // 2 :]
        out_ref[...] = (gate / (1.0 + jnp.exp(-gate)) * up).astype(BF16)

    return pl.pallas_call(
        body,
        out_shape=pltpu.VMEM((rows, cols // 2), BF16),
        in_specs=[VMEM] * 3,
        out_specs=VMEM,
        name="hidden",
    )(keep, square, *in_vmem(sent))


def down_terms(place, hidden, other, weights, give):
    n, rows = len(weights), hidden.shape[0]
    depth, cols = weights[0].shape

    def body(place_ref, hidden_ref, other_ref, *refs):
        weights, out_ref, w, sem = refs[:n], refs[n], refs[n + 1], refs[n + 2]
        copies = [
            pltpu.make_async_copy(weights[k], w.at[k], sem.at[k]) for k in range(n)
        ]
        for copy in copies:
            copy.start()
        same = place_ref[0] == place_ref[3]
        own = jnp.logical_not(same) if give else same
        lhs = jnp.where(own, hidden_ref[...], other_ref[...])
        for k in range(n):
            copies[k].wait()
            out_ref[k] = dot(lhs, w[k]).astype(out_ref.dtype)

    return pl.pallas_call(
        body,
        out_shape=pltpu.VMEM((n, rows, cols), BF16 if give else F32),
        in_specs=[SMEM, VMEM, VMEM] + [HBM] * n,
        out_specs=VMEM,
        scratch_shapes=[pltpu.VMEM((n, depth, cols), BF16), pltpu.SemaphoreType.DMA((n,))],
        name="down_give" if give else "down_keep",
    )(place, *in_vmem(hidden, other), *weights)


def rope_tables(positions):
    half = HD // 2
    frequency = THETA ** (-jnp.arange(half, dtype=F32) * 2.0 / HD)
    angles = positions.astype(F32)[:, None] * frequency[None, :]
    return jnp.cos(angles), jnp.sin(angles)


def pick(array, index, axis=0):
    return lax.dynamic_index_in_dim(array, index, axis, keepdims=False)


def from_x(array, r):
    return lax.ppermute(array, "x", [(i, (i - r) % NX) for i in range(NX)])


def project(place, pieces, gains, w_query, w_keyval, sums):
    arrays = [piece for piece, _, _ in pieces]
    n_z, rows, width = arrays[0].shape
    n_q, n_kv = w_query.shape[1], w_keyval.shape[0]
    steps = n_z * len(arrays)
    last = sums is not None

    def body(place_ref, gain_ref, wq_hbm, wkv_hbm, *refs):
        refs, rest = refs[: len(arrays)], refs[len(arrays) :]
        before, rest = (rest[:3], rest[3:]) if last else (None, rest)
        q_ref, kv_ref, sq_ref, wq, wkv, sem_q, sem_kv = rest

        def at(i):
            _, s, rc = pieces[i // n_z]
            return ((place_ref[0] ^ rc) * n_z + i % n_z) * 4 + (place_ref[1] ^ s)

        def copies(i):
            g = at(i) * width
            return (
                pltpu.make_async_copy(wq_hbm.at[pl.ds(g, width)], wq.at[i], sem_q.at[i]),
                pltpu.make_async_copy(wkv_hbm.at[:, pl.ds(g, width)], wkv.at[i], sem_kv.at[i]),
            )

        for i in range(steps):
            for copy in copies(i):
                copy.start()
        if last:
            for ref, old in zip((q_ref, kv_ref, sq_ref), before):
                ref[...] = old[...]
        else:
            for ref in (q_ref, kv_ref, sq_ref):
                ref[...] = jnp.zeros(ref.shape, F32)
        for p, ref in enumerate(refs):
            q, kv = q_ref[...], kv_ref[...]
            for r in range(n_z):
                i = p * n_z + r
                piece = ref[r].astype(F32)
                lhs = (piece * gain_ref[at(i)]).astype(BF16)
                sq_ref[...] += piece * piece
                for copy in copies(i):
                    copy.wait()
                q, kv = q + dot(lhs, wq[i]), kv + dot_t(wkv[i], lhs)
            q_ref[...], kv_ref[...] = q, kv
        if last:
            mean = jnp.sum(sq_ref[...], axis=1, keepdims=True) / (32 * width)
            factor = lax.rsqrt(mean + EPS)
            q_ref[...] = q_ref[...] * factor
            across = jnp.broadcast_to(factor, (rows, rows)).T[:1]
            kv_ref[...] = kv_ref[...] * across

    shapes = [(rows, n_q), (n_kv, rows), (rows, width)]
    return pl.pallas_call(
        body,
        out_shape=[pltpu.VMEM(shape, F32) for shape in shapes],
        in_specs=[SMEM, VMEM, HBM, HBM] + [VMEM] * (len(arrays) + (3 if last else 0)),
        out_specs=[VMEM] * 3,
        scratch_shapes=[
            pltpu.VMEM((steps, width, n_q), BF16),
            pltpu.VMEM((steps, n_kv, width), BF16),
            pltpu.SemaphoreType.DMA((steps,)),
            pltpu.SemaphoreType.DMA((steps,)),
        ],
        name="project_last" if last else "project_first",
    )(place, *in_vmem(gains), w_query, w_keyval, *in_vmem(*arrays, *(sums or ())))


def summed(terms, sent):
    quarter = terms.shape[1] // 4

    def both(s):
        rows = slice(s * quarter, (s + 1) * quarter)
        return terms[:, rows] + sent[:, rows].astype(F32)

    got = [from_sq(both(s).astype(BF16), s) for s in (1, 2, 3)]
    mine = both(0) + sum(t.astype(F32) for t in got)
    tiles = exchange(mine.astype(BF16), "zh")
    return tiles.astype(F32).sum(axis=0)


def gathered(piece):
    near = to_all(piece, "zh")
    ours = [near] + [from_sq(near, s) for s in (1, 2, 3)]
    theirs = [lax.ppermute(t, "c", SWAP) for t in ours]
    return ours, theirs


def layer(tokens_in, gain_attn, w_query, w_keyval, w_out, gain_mlp, w_gate, w_up, w_down):
    core, y_hi, x = lax.axis_index("c"), lax.axis_index("yh"), lax.axis_index("x")
    z_hi, z_lo, y_lo = lax.axis_index("zh"), lax.axis_index("zl"), lax.axis_index("yl")
    block, spot = lax.axis_index(DP), z_lo * 2 + y_lo
    rows, width = tokens_in.shape
    n_dp, n_z = lax.axis_size(DP), lax.axis_size(Z)
    dim = w_query.shape[0]
    block_d = dim // 8
    total = rows * n_dp
    quarter = rows // 4

    gate_up_w = jnp.concatenate([w_gate, w_up], axis=1)
    gate_up_next, gate_up_last = from_x(gate_up_w, 1), from_x(gate_up_w, 3)
    gate_up_all = [gate_up_w, gate_up_next, from_x(gate_up_w, 2), gate_up_last]
    down_next, down_last = from_x(w_down, 1), from_x(w_down, 3)
    down_all = [w_down, down_next, from_x(w_down, 2), down_last]

    ours, theirs = gathered(tokens_in)
    place = jnp.stack([core, spot, x, y_hi]).astype(jnp.int32)
    gains = gain_attn.astype(F32).reshape(4 * n_z, 1, width)
    pieces = [(t, s, rc) for rc, side in ((0, ours), (1, theirs)) for s, t in enumerate(side)]
    early = [p for p in pieces if p[1] == 0]
    late = [p for p in pieces if p[1] != 0]
    w_kv = w_keyval.T
    sums = project(place, early, gains, w_query, w_kv, None)
    query, kv_part, _ = project(place, late, gains, w_query, w_kv, sums)

    kv_here = move(
        kv_part.astype(BF16),
        lambda c, zh, zl, **_: {"c": zh // 2, "zh": (zh % 2) * 2 + zl, "zl": c},
    )
    parts = to_all(kv_here, ("yh", "x", "zl", "yl")).reshape(n_dp, 2, HD, rows)
    key_t = jnp.moveaxis(parts[:, 0], 0, 1).reshape(HD, total)
    value_t = jnp.moveaxis(parts[:, 1], 0, 1).reshape(HD, total)

    key_pos = jnp.arange(total, dtype=jnp.int32)
    cos_k, sin_k = rope_tables(key_pos)
    cos_k, sin_k = cos_k.T, sin_k.T
    k1, k2 = key_t[: HD // 2].astype(F32), key_t[HD // 2 :].astype(F32)
    key_rot = jnp.concatenate(
        [k1 * cos_k - k2 * sin_k, k2 * cos_k + k1 * sin_k], axis=0
    ).astype(BF16)
    pos = block * rows + jnp.arange(rows, dtype=jnp.int32)
    cos_q, sin_q = rope_tables(pos)
    heads = w_query.shape[1] // HD
    q_rot = []
    for h in range(heads):
        q1 = query[:, h * HD : h * HD + HD // 2]
        q2 = query[:, h * HD + HD // 2 : (h + 1) * HD]
        q_rot.append(jnp.concatenate([q1 * cos_q - q2 * sin_q, q2 * cos_q + q1 * sin_q], axis=1))
    q_rot = jnp.concatenate(q_rot, axis=0).astype(BF16)
    scores = dot(q_rot, key_rot) * HD ** (-0.5)
    allowed = key_pos[None, :] <= jnp.tile(pos, heads)[:, None]
    scores = jnp.where(allowed, scores, -1e30)
    expo = jnp.exp(scores - jnp.max(scores, axis=-1, keepdims=True))
    probs = (expo / jnp.sum(expo, axis=-1, keepdims=True)).astype(BF16)
    attended = lax.dot_general(
        probs, value_t, (((1,), (1,)), ((), ())), preferred_element_type=F32
    ).astype(BF16)
    sent = lax.ppermute(out_terms(place, attended, w_out, True), "c", SWAP)
    terms = out_terms(place, attended, w_out, False)
    resid = [
        lax.dynamic_slice(t, ((x + z_hi) % NX, spot * quarter, 0), (1, quarter, width))[0]
        for t in ours
    ]
    resid = jnp.stack(resid, axis=0)
    resid = jnp.concatenate([pick(resid, j ^ spot) for j in range(4)], axis=1)
    mid_part = (resid.astype(F32) + summed(terms, sent)).astype(BF16)
    mid_own = move(mid_part, lambda c, yh, **_: {"c": yh, "yh": c})

    ours, theirs = gathered(mid_own)

    gains_mlp = gain_mlp.astype(F32).reshape(n_dp, 1, block_d)
    sent, keep, square = gate_up_terms(place, gains_mlp, ours + theirs, gate_up_all)
    sent = lax.ppermute(sent, "yh", SWAP)
    hidden = hidden_units(keep, square, sent, dim)

    other = lax.ppermute(hidden, "yh", SWAP)
    sent = down_terms(place, hidden, other, down_all, True)
    sent = lax.ppermute(sent, "c", SWAP)
    terms = down_terms(place, hidden, other, down_all, False)
    done = (mid_own.astype(F32) + summed(terms, sent)).astype(BF16)
    return move(done, lambda x, zh, **_: {"x": (x + zh) % NX, "zh": x})


def solution(mesh):
    fine = Mesh(mesh.devices.reshape(SIZES), EVERY)
    placed = (
        P(DP, GROUP),
        P(),
        P(None, GROUP),
        P(None, GROUP),
        P(GROUP, None),
        P(),
        P(DP, GROUP),
        P(DP, GROUP),
        P(GROUP, DP),
    )
    return jax.shard_map(layer, mesh=fine, in_specs=placed, out_specs=P(GROUP, DP), check_vma=False)
```

```python
import jax
import jax.numpy as jnp
from jax import lax
from jax.experimental import pallas as pl
from jax.experimental.pallas import tpu as pltpu
from jax.sharding import Mesh
from jax.sharding import PartitionSpec as P


HD = 128
EPS = 1e-05
THETA = 10000.0

F32 = jnp.float32
BF16 = jnp.bfloat16
DP = ("yh", "x")
Z = ("zh", "zl")
GROUP = ("c", "zh", "zl", "yl")
EVERY = ("c", "yh", "x", "zh", "zl", "yl")
SIZES = (2, 2, 4, 4, 2, 2)
SWAP = [(0, 1), (1, 0)]
NX = 4


def dot(a, b):
    return jnp.dot(a, b, preferred_element_type=F32)


def dot_t(a, b):
    return lax.dot_general(a, b, (((1,), (1,)), ((), ())), preferred_element_type=F32)


def to_all(array, axis):
    length = lax.axis_size(axis)
    return exchange(jnp.broadcast_to(array[None], (length, *array.shape)), axis)


def exchange(tiles, axis):
    return lax.all_to_all(tiles, axis, 0, 0, tiled=True)


def from_sq(array, s):
    return lax.ppermute(array, ("zl", "yl"), [(i, i ^ s) for i in range(4)])


def move(array, target):
    moves = []
    for n in range(256):
        at, rest = {}, n
        for name, size in zip(reversed(EVERY), reversed(SIZES)):
            at[name] = rest % size
            rest //= size
        goal, to = {**at, **target(**at)}, 0
        for name, size in zip(EVERY, SIZES):
            to = to * size + goal[name]
        moves.append((n, to))
    return lax.ppermute(array, EVERY, moves)


VMEM = pl.BlockSpec(memory_space=pltpu.VMEM)
SMEM = pl.BlockSpec(memory_space=pltpu.SMEM)
HBM = pl.BlockSpec(memory_space=pl.ANY)


def in_vmem(*arrays):
    return [pltpu.with_memory_space_constraint(t, pltpu.VMEM) for t in arrays]


def out_terms(place, attended, w_out, give):
    depth, block = w_out.shape[0], w_out.shape[1] // (2 * NX)
    heads = depth // HD
    rows = attended.shape[0] // heads
    quarter = rows // 4

    def body(place_ref, lhs_ref, w_hbm, out_ref, w, sem):
        half = 1 - place_ref[0] if give else place_ref[0]

        def copy(k):
            at = (half * NX + (place_ref[2] + k) % NX) * block
            return pltpu.make_async_copy(w_hbm.at[:, pl.ds(at, block)], w.at[k], sem.at[k])

        for k in range(NX):
            copy(k).start()
        lhs = []
        for s in range(4):
            at = (place_ref[1] ^ s) * quarter
            parts = [lhs_ref[pl.ds(h * rows + at, quarter)] for h in range(heads)]
            lhs.append(jnp.concatenate(parts, axis=1))
        lhs = jnp.concatenate(lhs, axis=0)
        for k in range(NX):
            copy(k).wait()
            out_ref[k] = dot(lhs, w[k]).astype(out_ref.dtype)

    return pl.pallas_call(
        body,
        out_shape=pltpu.VMEM((NX, rows, block), BF16 if give else F32),
        in_specs=[SMEM, VMEM, HBM],
        out_specs=VMEM,
        scratch_shapes=[
            pltpu.VMEM((NX, depth, block), BF16),
            pltpu.SemaphoreType.DMA((NX,)),
        ],
        name="out_give" if give else "out_keep",
    )(place, *in_vmem(attended), w_out)


def gate_up_terms(place, gains, pieces, gates, ups):
    n, part, depth = pieces[0].shape
    rows, hid, count = 4 * part, gates[0].shape[1], len(pieces)
    cols = 2 * hid

    def body(place_ref, gain_ref, *refs):
        pieces, refs = refs[:count], refs[count:]
        gates, ups, refs = refs[:n], refs[n : 2 * n], refs[2 * n :]
        give_ref, keep_ref, square_ref, w, acc, sq, sem = refs
        copies = [
            (
                pltpu.make_async_copy(gates[k], w.at[k, :, pl.ds(0, hid)], sem.at[2 * k]),
                pltpu.make_async_copy(ups[k], w.at[k, :, pl.ds(hid, hid)], sem.at[2 * k + 1]),
            )
            for k in range(n)
        ]
        for pair in copies:
            for copy in pair:
                copy.start()
        for k in range(n):
            lhs = jnp.concatenate([p[k] for p in pieces], axis=0)
            wide = lhs.astype(F32)
            square = jnp.sum(wide * wide, axis=1, keepdims=True)
            for copy in copies[k]:
                copy.wait()
            gain = gain_ref[place_ref[3] * n + (place_ref[2] + k) % n]
            out = dot((wide * gain).astype(BF16), w[k])
            if k == 0:
                acc[...], sq[...] = out, jnp.broadcast_to(square, sq.shape)
            else:
                acc[...] += out
                sq[...] += square
        keep = pl.multiple_of((place_ref[3] ^ place_ref[0]) * rows, rows)
        give = pl.multiple_of(((1 - place_ref[3]) ^ place_ref[0]) * rows, rows)
        give_ref[:, :cols] = acc[pl.ds(give, rows)].astype(BF16)
        square = sq[pl.ds(give, rows)]
        top = square.astype(BF16)
        low = (square - top.astype(F32)).astype(BF16)
        lane = lax.broadcasted_iota(jnp.int32, square.shape, 1)
        give_ref[:, cols:] = jnp.where(lane == 0, top.astype(F32), low.astype(F32)).astype(BF16)
        keep_ref[...] = acc[pl.ds(keep, rows)]
        square_ref[...] = sq[pl.ds(keep, rows)]

    return pl.pallas_call(
        body,
        out_shape=[
            pltpu.VMEM((rows, cols + 128), BF16),
            jax.ShapeDtypeStruct((rows, cols), F32),
            jax.ShapeDtypeStruct((rows, 128), F32),
        ],
        in_specs=[SMEM, VMEM] + [VMEM] * count + [HBM] * (2 * n),
        out_specs=[VMEM] * 3,
        scratch_shapes=[
            pltpu.VMEM((n, depth, cols), BF16),
            pltpu.VMEM((2 * rows, cols), F32),
            pltpu.VMEM((2 * rows, 128), F32),
            pltpu.SemaphoreType.DMA((2 * n,)),
        ],
        name="gate_up",
    )(place, gains, *in_vmem(*pieces), *gates, *ups)


def hidden_units(keep, square, sent, dim):
    rows, cols = keep.shape

    def body(keep_ref, square_ref, sent_ref, out_ref):
        extra = sent_ref[:, cols:].astype(F32)
        mean = (square_ref[:, :1] + extra[:, :1] + extra[:, 1:2]) / dim
        out = (keep_ref[...] + sent_ref[:, :cols].astype(F32)) * lax.rsqrt(mean + EPS)
        gate, up = out[:, : cols // 2], out[:, cols // 2 :]
        out_ref[...] = (gate / (1.0 + jnp.exp(-gate)) * up).astype(BF16)

    return pl.pallas_call(
        body,
        out_shape=pltpu.VMEM((rows, cols // 2), BF16),
        in_specs=[VMEM] * 3,
        out_specs=VMEM,
        name="hidden",
    )(keep, square, *in_vmem(sent))


def down_terms(place, hidden, other, weights, give):
    n, rows = len(weights), hidden.shape[0]
    depth, cols = weights[0][0].shape
    arrays = [(t, k, i * t.shape[0]) for k, parts in enumerate(weights) for i, t in enumerate(parts)]
    count = len(arrays)

    def body(place_ref, hidden_ref, other_ref, *refs):
        weights, out_ref, w, sem = refs[:count], refs[count], refs[count + 1], refs[count + 2]
        copies = [
            pltpu.make_async_copy(ref, w.at[k, pl.ds(at, t.shape[0])], sem.at[i])
            for i, (ref, (t, k, at)) in enumerate(zip(weights, arrays))
        ]
        for copy in copies:
            copy.start()
        same = place_ref[0] == place_ref[3]
        own = jnp.logical_not(same) if give else same
        lhs = jnp.where(own, hidden_ref[...], other_ref[...])
        for k in range(n):
            for copy, (_, owner, _) in zip(copies, arrays):
                if owner == k:
                    copy.wait()
            out_ref[k] = dot(lhs, w[k]).astype(out_ref.dtype)

    return pl.pallas_call(
        body,
        out_shape=pltpu.VMEM((n, rows, cols), BF16 if give else F32),
        in_specs=[SMEM, VMEM, VMEM] + [HBM] * count,
        out_specs=VMEM,
        scratch_shapes=[pltpu.VMEM((n, depth, cols), BF16), pltpu.SemaphoreType.DMA((count,))],
        name="down_give" if give else "down_keep",
    )(place, *in_vmem(hidden, other), *[t for t, _, _ in arrays])


def rope_tables(positions):
    half = HD // 2
    frequency = THETA ** (-jnp.arange(half, dtype=F32) * 2.0 / HD)
    angles = positions.astype(F32)[:, None] * frequency[None, :]
    return jnp.cos(angles), jnp.sin(angles)


def pick(array, index, axis=0):
    return lax.dynamic_index_in_dim(array, index, axis, keepdims=False)


def from_x(array, r):
    return lax.ppermute(array, "x", [(i, (i - r) % NX) for i in range(NX)])


def project(place, pieces, gains, w_query, w_keyval, sums):
    arrays = [piece for piece, _, _ in pieces]
    n_z, rows, width = arrays[0].shape
    n_q, n_kv = w_query.shape[1], w_keyval.shape[0]
    steps = n_z * len(arrays)
    last = sums is not None

    def body(place_ref, gain_ref, wq_hbm, wkv_hbm, *refs):
        refs, rest = refs[: len(arrays)], refs[len(arrays) :]
        before, rest = (rest[:3], rest[3:]) if last else (None, rest)
        q_ref, kv_ref, sq_ref, wq, wkv, sem_q, sem_kv = rest

        def at(i):
            _, s, rc = pieces[i // n_z]
            return ((place_ref[0] ^ rc) * n_z + i % n_z) * 4 + (place_ref[1] ^ s)

        def copies(i):
            g = at(i) * width
            return (
                pltpu.make_async_copy(wq_hbm.at[pl.ds(g, width)], wq.at[i], sem_q.at[i]),
                pltpu.make_async_copy(wkv_hbm.at[:, pl.ds(g, width)], wkv.at[i], sem_kv.at[i]),
            )

        for i in range(steps):
            for copy in copies(i):
                copy.start()
        if last:
            for ref, old in zip((q_ref, kv_ref, sq_ref), before):
                ref[...] = old[...]
        else:
            for ref in (q_ref, kv_ref, sq_ref):
                ref[...] = jnp.zeros(ref.shape, F32)
        for p, ref in enumerate(refs):
            q, kv = q_ref[...], kv_ref[...]
            for r in range(n_z):
                i = p * n_z + r
                piece = ref[r].astype(F32)
                lhs = (piece * gain_ref[at(i)]).astype(BF16)
                sq_ref[...] += piece * piece
                for copy in copies(i):
                    copy.wait()
                q, kv = q + dot(lhs, wq[i]), kv + dot_t(wkv[i], lhs)
            q_ref[...], kv_ref[...] = q, kv
        if last:
            mean = jnp.sum(sq_ref[...], axis=1, keepdims=True) / (32 * width)
            factor = lax.rsqrt(mean + EPS)
            q_ref[...] = q_ref[...] * factor
            across = jnp.broadcast_to(factor, (rows, rows)).T[:1]
            kv_ref[...] = kv_ref[...] * across

    shapes = [(rows, n_q), (n_kv, rows), (rows, width)]
    return pl.pallas_call(
        body,
        out_shape=[pltpu.VMEM(shape, F32) for shape in shapes],
        in_specs=[SMEM, VMEM, HBM, HBM] + [VMEM] * (len(arrays) + (3 if last else 0)),
        out_specs=[VMEM] * 3,
        scratch_shapes=[
            pltpu.VMEM((steps, width, n_q), BF16),
            pltpu.VMEM((steps, n_kv, width), BF16),
            pltpu.SemaphoreType.DMA((steps,)),
            pltpu.SemaphoreType.DMA((steps,)),
        ],
        name="project_last" if last else "project_first",
    )(place, *in_vmem(gains), w_query, w_keyval, *in_vmem(*arrays, *(sums or ())))


def summed(terms, sent):
    quarter = terms.shape[1] // 4

    def both(s):
        rows = slice(s * quarter, (s + 1) * quarter)
        return terms[:, rows] + sent[:, rows].astype(F32)

    got = [from_sq(both(s).astype(BF16), s) for s in (1, 2, 3)]
    mine = both(0) + sum(t.astype(F32) for t in got)
    tiles = exchange(mine.astype(BF16), "zh")
    return tiles.astype(F32).sum(axis=0)


def gathered(piece):
    near = to_all(piece, "zh")
    ours = [near] + [from_sq(near, s) for s in (1, 2, 3)]
    theirs = [lax.ppermute(t, "c", SWAP) for t in ours]
    return ours, theirs


def layer(tokens_in, gain_attn, w_query, w_keyval, w_out, gain_mlp, w_gate, w_up, w_down):
    core, y_hi, x = lax.axis_index("c"), lax.axis_index("yh"), lax.axis_index("x")
    z_hi, z_lo, y_lo = lax.axis_index("zh"), lax.axis_index("zl"), lax.axis_index("yl")
    block, spot = lax.axis_index(DP), z_lo * 2 + y_lo
    rows, width = tokens_in.shape
    n_dp, n_z = lax.axis_size(DP), lax.axis_size(Z)
    dim = w_query.shape[0]
    block_d = dim // 8
    total = rows * n_dp
    quarter = rows // 4
    hid = w_gate.shape[1]

    gate_next, gate_last = from_x(w_gate, 1), from_x(w_gate, 3)
    up_next, up_last = from_x(w_up, 1), from_x(w_up, 3)
    gate_all = [w_gate, gate_next, from_x(gate_next, 1), gate_last]
    up_all = [w_up, up_next, from_x(up_last, 3), up_last]
    down_next, down_last = from_x(w_down, 1), from_x(w_down, 3)
    part = hid // 2
    down_far = (from_x(down_next[:part], 1), from_x(down_last[part:], 3))
    down_all = [(w_down,), (down_next,), down_far, (down_last,)]

    ours, theirs = gathered(tokens_in)
    place = jnp.stack([core, spot, x, y_hi]).astype(jnp.int32)
    gains = gain_attn.astype(F32).reshape(4 * n_z, 1, width)
    pieces = [(t, s, rc) for rc, side in ((0, ours), (1, theirs)) for s, t in enumerate(side)]
    early = [p for p in pieces if p[1] == 0]
    late = [p for p in pieces if p[1] != 0]
    w_kv = w_keyval.T
    sums = project(place, early, gains, w_query, w_kv, None)
    query, kv_part, _ = project(place, late, gains, w_query, w_kv, sums)

    kv_here = move(
        kv_part.astype(BF16),
        lambda c, zh, zl, **_: {"c": zh // 2, "zh": (zh % 2) * 2 + zl, "zl": c},
    )
    parts = to_all(kv_here, ("yh", "x", "zl", "yl")).reshape(n_dp, 2, HD, rows)
    key_t = jnp.moveaxis(parts[:, 0], 0, 1).reshape(HD, total)
    value_t = jnp.moveaxis(parts[:, 1], 0, 1).reshape(HD, total)

    key_pos = jnp.arange(total, dtype=jnp.int32)
    cos_k, sin_k = rope_tables(key_pos)
    cos_k, sin_k = cos_k.T, sin_k.T
    k1, k2 = key_t[: HD // 2].astype(F32), key_t[HD // 2 :].astype(F32)
    key_rot = jnp.concatenate(
        [k1 * cos_k - k2 * sin_k, k2 * cos_k + k1 * sin_k], axis=0
    ).astype(BF16)
    pos = block * rows + jnp.arange(rows, dtype=jnp.int32)
    cos_q, sin_q = rope_tables(pos)
    heads = w_query.shape[1] // HD
    q_rot = []
    for h in range(heads):
        q1 = query[:, h * HD : h * HD + HD // 2]
        q2 = query[:, h * HD + HD // 2 : (h + 1) * HD]
        q_rot.append(jnp.concatenate([q1 * cos_q - q2 * sin_q, q2 * cos_q + q1 * sin_q], axis=1))
    q_rot = jnp.concatenate(q_rot, axis=0).astype(BF16)
    scores = dot(q_rot, key_rot) * HD ** (-0.5)
    allowed = key_pos[None, :] <= jnp.tile(pos, heads)[:, None]
    scores = jnp.where(allowed, scores, -1e30)
    expo = jnp.exp(scores - jnp.max(scores, axis=-1, keepdims=True))
    probs = (expo / jnp.sum(expo, axis=-1, keepdims=True)).astype(BF16)
    attended = lax.dot_general(
        probs, value_t, (((1,), (1,)), ((), ())), preferred_element_type=F32
    ).astype(BF16)
    sent = lax.ppermute(out_terms(place, attended, w_out, True), "c", SWAP)
    terms = out_terms(place, attended, w_out, False)
    resid = [
        lax.dynamic_slice(t, ((x + z_hi) % NX, spot * quarter, 0), (1, quarter, width))[0]
        for t in ours
    ]
    resid = jnp.stack(resid, axis=0)
    resid = jnp.concatenate([pick(resid, j ^ spot) for j in range(4)], axis=1)
    mid_part = (resid.astype(F32) + summed(terms, sent)).astype(BF16)
    mid_own = move(mid_part, lambda c, yh, **_: {"c": yh, "yh": c})

    ours, theirs = gathered(mid_own)

    gains_mlp = gain_mlp.astype(F32).reshape(n_dp, 1, block_d)
    sent, keep, square = gate_up_terms(place, gains_mlp, ours + theirs, gate_all, up_all)
    sent = lax.ppermute(sent, "yh", SWAP)
    hidden = hidden_units(keep, square, sent, dim)

    other = lax.ppermute(hidden, "yh", SWAP)
    sent = down_terms(place, hidden, other, down_all, True)
    sent = lax.ppermute(sent, "c", SWAP)
    terms = down_terms(place, hidden, other, down_all, False)
    done = (mid_own.astype(F32) + summed(terms, sent)).astype(BF16)
    return move(done, lambda x, zh, **_: {"x": (x + zh) % NX, "zh": x})


def solution(mesh):
    fine = Mesh(mesh.devices.reshape(SIZES), EVERY)
    placed = (
        P(DP, GROUP),
        P(),
        P(None, GROUP),
        P(None, GROUP),
        P(GROUP, None),
        P(),
        P(DP, GROUP),
        P(DP, GROUP),
        P(GROUP, DP),
    )
    return jax.shard_map(layer, mesh=fine, in_specs=placed, out_specs=P(GROUP, DP), check_vma=False)
```

```python
import jax
import jax.numpy as jnp
from jax import lax
from jax.experimental import pallas as pl
from jax.experimental.pallas import tpu as pltpu
from jax.sharding import Mesh
from jax.sharding import PartitionSpec as P


HD = 128
EPS = 1e-05
THETA = 10000.0

F32 = jnp.float32
BF16 = jnp.bfloat16
DP = ("yh", "x")
Z = ("zh", "zl")
GROUP = ("c", "zh", "zl", "yl")
EVERY = ("c", "yh", "x", "zh", "zl", "yl")
SIZES = (2, 2, 4, 4, 2, 2)
SWAP = [(0, 1), (1, 0)]
NX = 4


def dot(a, b):
    return jnp.dot(a, b, preferred_element_type=F32)


def dot_t(a, b):
    return lax.dot_general(a, b, (((1,), (1,)), ((), ())), preferred_element_type=F32)


def to_all(array, axis):
    length = lax.axis_size(axis)
    return exchange(jnp.broadcast_to(array[None], (length, *array.shape)), axis)


def exchange(tiles, axis):
    return lax.all_to_all(tiles, axis, 0, 0, tiled=True)


def from_sq(array, s):
    return lax.ppermute(array, ("zl", "yl"), [(i, i ^ s) for i in range(4)])


def move(array, target):
    moves = []
    for n in range(256):
        at, rest = {}, n
        for name, size in zip(reversed(EVERY), reversed(SIZES)):
            at[name] = rest % size
            rest //= size
        goal, to = {**at, **target(**at)}, 0
        for name, size in zip(EVERY, SIZES):
            to = to * size + goal[name]
        moves.append((n, to))
    return lax.ppermute(array, EVERY, moves)


VMEM = pl.BlockSpec(memory_space=pltpu.VMEM)
SMEM = pl.BlockSpec(memory_space=pltpu.SMEM)
HBM = pl.BlockSpec(memory_space=pl.ANY)


def in_vmem(*arrays):
    return [pltpu.with_memory_space_constraint(t, pltpu.VMEM) for t in arrays]


def out_terms(place, attended, w_out, give):
    depth, block = w_out.shape[0], w_out.shape[1] // (2 * NX)
    heads = depth // HD
    rows = attended.shape[0] // heads
    quarter = rows // 4

    def body(place_ref, lhs_ref, w_hbm, out_ref, w, sem):
        half = 1 - place_ref[0] if give else place_ref[0]

        def copy(k):
            at = (half * NX + (place_ref[2] + k) % NX) * block
            return pltpu.make_async_copy(w_hbm.at[:, pl.ds(at, block)], w.at[k], sem.at[k])

        for k in range(NX):
            copy(k).start()
        lhs = []
        for s in range(4):
            at = (place_ref[1] ^ s) * quarter
            parts = [lhs_ref[pl.ds(h * rows + at, quarter)] for h in range(heads)]
            lhs.append(jnp.concatenate(parts, axis=1))
        lhs = jnp.concatenate(lhs, axis=0)
        for k in range(NX):
            copy(k).wait()
            out_ref[k] = dot(lhs, w[k]).astype(out_ref.dtype)

    return pl.pallas_call(
        body,
        out_shape=pltpu.VMEM((NX, rows, block), BF16 if give else F32),
        in_specs=[SMEM, VMEM, HBM],
        out_specs=VMEM,
        scratch_shapes=[
            pltpu.VMEM((NX, depth, block), BF16),
            pltpu.SemaphoreType.DMA((NX,)),
        ],
        name="out_give" if give else "out_keep",
    )(place, *in_vmem(attended), w_out)


def gate_up_terms(place, gains, pieces, gates, ups):
    n, part, depth = pieces[0].shape
    rows, hid, count = 4 * part, gates[0].shape[1], len(pieces)
    cols = 2 * hid

    def body(place_ref, gain_ref, *refs):
        pieces, refs = refs[:count], refs[count:]
        gates, ups, refs = refs[:n], refs[n : 2 * n], refs[2 * n :]
        give_ref, keep_ref, square_ref, w, acc, sq, sem = refs
        copies = [
            (
                pltpu.make_async_copy(gates[k], w.at[k, :, pl.ds(0, hid)], sem.at[2 * k]),
                pltpu.make_async_copy(ups[k], w.at[k, :, pl.ds(hid, hid)], sem.at[2 * k + 1]),
            )
            for k in range(n)
        ]
        for pair in copies:
            for copy in pair:
                copy.start()
        for k in range(n):
            lhs = jnp.concatenate([p[k] for p in pieces], axis=0)
            wide = lhs.astype(F32)
            square = jnp.sum(wide * wide, axis=1, keepdims=True)
            for copy in copies[k]:
                copy.wait()
            gain = gain_ref[place_ref[3] * n + (place_ref[2] + k) % n]
            out = dot((wide * gain).astype(BF16), w[k])
            if k == 0:
                acc[...], sq[...] = out, jnp.broadcast_to(square, sq.shape)
            else:
                acc[...] += out
                sq[...] += square
        keep = pl.multiple_of((place_ref[3] ^ place_ref[0]) * rows, rows)
        give = pl.multiple_of(((1 - place_ref[3]) ^ place_ref[0]) * rows, rows)
        give_ref[:, :cols] = acc[pl.ds(give, rows)].astype(BF16)
        square = sq[pl.ds(give, rows)]
        top = square.astype(BF16)
        low = (square - top.astype(F32)).astype(BF16)
        lane = lax.broadcasted_iota(jnp.int32, square.shape, 1)
        give_ref[:, cols:] = jnp.where(lane == 0, top.astype(F32), low.astype(F32)).astype(BF16)
        keep_ref[...] = acc[pl.ds(keep, rows)]
        square_ref[...] = sq[pl.ds(keep, rows)]

    return pl.pallas_call(
        body,
        out_shape=[
            pltpu.VMEM((rows, cols + 128), BF16),
            jax.ShapeDtypeStruct((rows, cols), F32),
            jax.ShapeDtypeStruct((rows, 128), F32),
        ],
        in_specs=[SMEM, VMEM] + [VMEM] * count + [HBM] * (2 * n),
        out_specs=[VMEM] * 3,
        scratch_shapes=[
            pltpu.VMEM((n, depth, cols), BF16),
            pltpu.VMEM((2 * rows, cols), F32),
            pltpu.VMEM((2 * rows, 128), F32),
            pltpu.SemaphoreType.DMA((2 * n,)),
        ],
        name="gate_up",
    )(place, gains, *in_vmem(*pieces), *gates, *ups)


def hidden_units(keep, square, sent, dim):
    rows, cols = keep.shape

    def body(keep_ref, square_ref, sent_ref, out_ref):
        extra = sent_ref[:, cols:].astype(F32)
        mean = (square_ref[:, :1] + extra[:, :1] + extra[:, 1:2]) / dim
        out = (keep_ref[...] + sent_ref[:, :cols].astype(F32)) * lax.rsqrt(mean + EPS)
        gate, up = out[:, : cols // 2], out[:, cols // 2 :]
        out_ref[...] = (gate / (1.0 + jnp.exp(-gate)) * up).astype(BF16)

    return pl.pallas_call(
        body,
        out_shape=pltpu.VMEM((rows, cols // 2), BF16),
        in_specs=[VMEM] * 3,
        out_specs=VMEM,
        name="hidden",
    )(keep, square, *in_vmem(sent))


def down_terms(place, hidden, other, weights, give):
    n, rows = len(weights), hidden.shape[0]
    depth, cols = weights[0].shape

    def body(place_ref, hidden_ref, other_ref, *refs):
        weights, out_ref, w, sem = refs[:n], refs[n], refs[n + 1], refs[n + 2]
        copies = [
            pltpu.make_async_copy(weights[k], w.at[k], sem.at[k]) for k in range(n)
        ]
        for copy in copies:
            copy.start()
        same = place_ref[0] == place_ref[3]
        own = jnp.logical_not(same) if give else same
        lhs = jnp.where(own, hidden_ref[...], other_ref[...])
        for k in range(n):
            copies[k].wait()
            out_ref[k] = dot(lhs, w[k]).astype(out_ref.dtype)

    return pl.pallas_call(
        body,
        out_shape=pltpu.VMEM((n, rows, cols), BF16 if give else F32),
        in_specs=[SMEM, VMEM, VMEM] + [HBM] * n,
        out_specs=VMEM,
        scratch_shapes=[pltpu.VMEM((n, depth, cols), BF16), pltpu.SemaphoreType.DMA((n,))],
        name="down_give" if give else "down_keep",
    )(place, *in_vmem(hidden, other), *weights)


def rope_tables(positions):
    half = HD // 2
    frequency = THETA ** (-jnp.arange(half, dtype=F32) * 2.0 / HD)
    angles = positions.astype(F32)[:, None] * frequency[None, :]
    return jnp.cos(angles), jnp.sin(angles)


def pick(array, index, axis=0):
    return lax.dynamic_index_in_dim(array, index, axis, keepdims=False)


def from_x(array, r):
    return lax.ppermute(array, "x", [(i, (i - r) % NX) for i in range(NX)])


def project(place, pieces, gains, w_query, w_keyval, sums):
    arrays = [piece for piece, _, _ in pieces]
    n_z, rows, width = arrays[0].shape
    n_q, n_kv = w_query.shape[1], w_keyval.shape[0]
    steps = n_z * len(arrays)
    last = sums is not None

    def body(place_ref, gain_ref, wq_hbm, wkv_hbm, *refs):
        refs, rest = refs[: len(arrays)], refs[len(arrays) :]
        before, rest = (rest[:3], rest[3:]) if last else (None, rest)
        q_ref, kv_ref, sq_ref, wq, wkv, sem_q, sem_kv = rest

        def at(i):
            _, s, rc = pieces[i // n_z]
            return ((place_ref[0] ^ rc) * n_z + i % n_z) * 4 + (place_ref[1] ^ s)

        def copies(i):
            g = at(i) * width
            return (
                pltpu.make_async_copy(wq_hbm.at[pl.ds(g, width)], wq.at[i], sem_q.at[i]),
                pltpu.make_async_copy(wkv_hbm.at[:, pl.ds(g, width)], wkv.at[i], sem_kv.at[i]),
            )

        for i in range(steps):
            for copy in copies(i):
                copy.start()
        if last:
            for ref, old in zip((q_ref, kv_ref, sq_ref), before):
                ref[...] = old[...]
        else:
            for ref in (q_ref, kv_ref, sq_ref):
                ref[...] = jnp.zeros(ref.shape, F32)
        for p, ref in enumerate(refs):
            q, kv = q_ref[...], kv_ref[...]
            for r in range(n_z):
                i = p * n_z + r
                piece = ref[r].astype(F32)
                lhs = (piece * gain_ref[at(i)]).astype(BF16)
                sq_ref[...] += piece * piece
                for copy in copies(i):
                    copy.wait()
                q, kv = q + dot(lhs, wq[i]), kv + dot_t(wkv[i], lhs)
            q_ref[...], kv_ref[...] = q, kv
        if last:
            mean = jnp.sum(sq_ref[...], axis=1, keepdims=True) / (32 * width)
            factor = lax.rsqrt(mean + EPS)
            q_ref[...] = q_ref[...] * factor
            across = jnp.broadcast_to(factor, (rows, rows)).T[:1]
            kv_ref[...] = kv_ref[...] * across

    shapes = [(rows, n_q), (n_kv, rows), (rows, width)]
    return pl.pallas_call(
        body,
        out_shape=[pltpu.VMEM(shape, F32) for shape in shapes],
        in_specs=[SMEM, VMEM, HBM, HBM] + [VMEM] * (len(arrays) + (3 if last else 0)),
        out_specs=[VMEM] * 3,
        scratch_shapes=[
            pltpu.VMEM((steps, width, n_q), BF16),
            pltpu.VMEM((steps, n_kv, width), BF16),
            pltpu.SemaphoreType.DMA((steps,)),
            pltpu.SemaphoreType.DMA((steps,)),
        ],
        name="project_last" if last else "project_first",
    )(place, *in_vmem(gains), w_query, w_keyval, *in_vmem(*arrays, *(sums or ())))


def over_square(terms, sent):
    quarter = terms.shape[1] // 4

    def both(s):
        rows = slice(s * quarter, (s + 1) * quarter)
        return terms[:, rows] + sent[:, rows].astype(F32)

    got = [from_sq(both(s).astype(BF16), s) for s in (1, 2, 3)]
    return (both(0) + sum(t.astype(F32) for t in got)).astype(BF16)


def gathered(piece):
    near = to_all(piece, "zh")
    ours = [near] + [from_sq(near, s) for s in (1, 2, 3)]
    theirs = [lax.ppermute(t, "c", SWAP) for t in ours]
    return ours, theirs


def layer(tokens_in, gain_attn, w_query, w_keyval, w_out, gain_mlp, w_gate, w_up, w_down):
    core, y_hi, x = lax.axis_index("c"), lax.axis_index("yh"), lax.axis_index("x")
    z_hi, z_lo, y_lo = lax.axis_index("zh"), lax.axis_index("zl"), lax.axis_index("yl")
    block, spot = lax.axis_index(DP), z_lo * 2 + y_lo
    rows, width = tokens_in.shape
    n_dp, n_z = lax.axis_size(DP), lax.axis_size(Z)
    dim = w_query.shape[0]
    block_d = dim // 8
    total = rows * n_dp
    quarter = rows // 4

    gate_next, gate_last = from_x(w_gate, 1), from_x(w_gate, 3)
    up_next, up_last = from_x(w_up, 1), from_x(w_up, 3)
    gate_all = [w_gate, gate_next, from_x(gate_next, 1), gate_last]
    up_all = [w_up, up_next, from_x(up_last, 3), up_last]
    down_next, down_last = from_x(w_down, 1), from_x(w_down, 3)
    down_all = [w_down, down_next, from_x(down_next, 1), down_last]

    ours, theirs = gathered(tokens_in)
    place = jnp.stack([core, spot, x, y_hi]).astype(jnp.int32)
    gains = gain_attn.astype(F32).reshape(4 * n_z, 1, width)
    pieces = [(t, s, rc) for rc, side in ((0, ours), (1, theirs)) for s, t in enumerate(side)]
    early = [p for p in pieces if p[1] == 0]
    late = [p for p in pieces if p[1] != 0]
    w_kv = w_keyval.T
    sums = project(place, early, gains, w_query, w_kv, None)
    query, kv_part, _ = project(place, late, gains, w_query, w_kv, sums)

    kv_here = move(
        kv_part.astype(BF16),
        lambda c, zh, zl, **_: {"c": zh // 2, "zh": (zh % 2) * 2 + zl, "zl": c},
    )
    parts = to_all(kv_here, ("yh", "x", "zl", "yl")).reshape(n_dp, 2, HD, rows)
    key_t = jnp.moveaxis(parts[:, 0], 0, 1).reshape(HD, total)
    value_t = jnp.moveaxis(parts[:, 1], 0, 1).reshape(HD, total)

    key_pos = jnp.arange(total, dtype=jnp.int32)
    cos_k, sin_k = rope_tables(key_pos)
    cos_k, sin_k = cos_k.T, sin_k.T
    k1, k2 = key_t[: HD // 2].astype(F32), key_t[HD // 2 :].astype(F32)
    key_rot = jnp.concatenate(
        [k1 * cos_k - k2 * sin_k, k2 * cos_k + k1 * sin_k], axis=0
    ).astype(BF16)
    pos = block * rows + jnp.arange(rows, dtype=jnp.int32)
    cos_q, sin_q = rope_tables(pos)
    heads = w_query.shape[1] // HD
    q_rot = []
    for h in range(heads):
        q1 = query[:, h * HD : h * HD + HD // 2]
        q2 = query[:, h * HD + HD // 2 : (h + 1) * HD]
        q_rot.append(jnp.concatenate([q1 * cos_q - q2 * sin_q, q2 * cos_q + q1 * sin_q], axis=1))
    q_rot = jnp.concatenate(q_rot, axis=0).astype(BF16)
    scores = dot(q_rot, key_rot) * HD ** (-0.5)
    allowed = key_pos[None, :] <= jnp.tile(pos, heads)[:, None]
    scores = jnp.where(allowed, scores, -1e30)
    expo = jnp.exp(scores - jnp.max(scores, axis=-1, keepdims=True))
    probs = (expo / jnp.sum(expo, axis=-1, keepdims=True)).astype(BF16)
    attended = lax.dot_general(
        probs, value_t, (((1,), (1,)), ((), ())), preferred_element_type=F32
    ).astype(BF16)
    sent = lax.ppermute(out_terms(place, attended, w_out, True), "c", SWAP)
    terms = out_terms(place, attended, w_out, False)
    resid = [
        lax.dynamic_slice(t, ((x + z_hi) % NX, spot * quarter, 0), (1, quarter, width))[0]
        for t in ours
    ]
    resid = jnp.stack(resid, axis=0)
    resid = jnp.concatenate([pick(resid, j ^ spot) for j in range(4)], axis=1)
    tiles = over_square(terms, sent)
    tiles = exchange(tiles, "zh")
    mid_part = (resid.astype(F32) + tiles.astype(F32).sum(axis=0)).astype(BF16)
    mid_own = move(mid_part, lambda c, yh, **_: {"c": yh, "yh": c})

    ours, theirs = gathered(mid_own)

    resid = move(mid_own, lambda x, zh, **_: {"x": (x + zh) % NX, "zh": x})

    gains_mlp = gain_mlp.astype(F32).reshape(n_dp, 1, block_d)
    sent, keep, square = gate_up_terms(place, gains_mlp, ours + theirs, gate_all, up_all)
    sent = lax.ppermute(sent, "yh", SWAP)
    hidden = hidden_units(keep, square, sent, dim)

    other = lax.ppermute(hidden, "yh", SWAP)
    sent = down_terms(place, hidden, other, down_all, True)
    sent = lax.ppermute(sent, "c", SWAP)
    terms = down_terms(place, hidden, other, down_all, False)
    tiles = over_square(terms, sent)
    got = [
        move(
            pick(tiles, (z_hi + r) % NX),
            lambda x, zh, r=r, **_: {"x": (x + zh + r) % NX, "zh": x},
        )
        for r in range(NX)
    ]
    done = resid.astype(F32) + sum(t.astype(F32) for t in got)
    return done.astype(BF16)


def solution(mesh):
    fine = Mesh(mesh.devices.reshape(SIZES), EVERY)
    placed = (
        P(DP, GROUP),
        P(),
        P(None, GROUP),
        P(None, GROUP),
        P(GROUP, None),
        P(),
        P(DP, GROUP),
        P(DP, GROUP),
        P(GROUP, DP),
    )
    return jax.shard_map(layer, mesh=fine, in_specs=placed, out_specs=P(GROUP, DP), check_vma=False)
```

```python
import jax
import jax.numpy as jnp
from jax import lax
from jax.experimental import pallas as pl
from jax.experimental.pallas import tpu as pltpu
from jax.sharding import Mesh
from jax.sharding import PartitionSpec as P


HD = 128
EPS = 1e-05
THETA = 10000.0

F32 = jnp.float32
BF16 = jnp.bfloat16
DP = ("yh", "x")
Z = ("zh", "zl")
GROUP = ("c", "zh", "zl", "yl")
EVERY = ("c", "yh", "x", "zh", "zl", "yl")
SIZES = (2, 2, 4, 4, 2, 2)
SWAP = [(0, 1), (1, 0)]
NX = 4


def dot(a, b):
    return jnp.dot(a, b, preferred_element_type=F32)


def dot_t(a, b):
    return lax.dot_general(a, b, (((1,), (1,)), ((), ())), preferred_element_type=F32)


def to_all(array, axis):
    length = lax.axis_size(axis)
    return exchange(jnp.broadcast_to(array[None], (length, *array.shape)), axis)


def exchange(tiles, axis):
    return lax.all_to_all(tiles, axis, 0, 0, tiled=True)


def from_sq(array, s):
    return lax.ppermute(array, ("zl", "yl"), [(i, i ^ s) for i in range(4)])


def move(array, target):
    moves = []
    for n in range(256):
        at, rest = {}, n
        for name, size in zip(reversed(EVERY), reversed(SIZES)):
            at[name] = rest % size
            rest //= size
        goal, to = {**at, **target(**at)}, 0
        for name, size in zip(EVERY, SIZES):
            to = to * size + goal[name]
        moves.append((n, to))
    return lax.ppermute(array, EVERY, moves)


VMEM = pl.BlockSpec(memory_space=pltpu.VMEM)
SMEM = pl.BlockSpec(memory_space=pltpu.SMEM)
HBM = pl.BlockSpec(memory_space=pl.ANY)


def in_vmem(*arrays):
    return [pltpu.with_memory_space_constraint(t, pltpu.VMEM) for t in arrays]


def out_terms(place, attended, w_out, give):
    depth, block = w_out.shape[0], w_out.shape[1] // (2 * NX)
    heads = depth // HD
    rows = attended.shape[0] // heads
    quarter = rows // 4

    def body(place_ref, lhs_ref, w_hbm, out_ref, w, sem):
        half = 1 - place_ref[0] if give else place_ref[0]

        def copy(k):
            at = (half * NX + (place_ref[2] + k) % NX) * block
            return pltpu.make_async_copy(w_hbm.at[:, pl.ds(at, block)], w.at[k], sem.at[k])

        for k in range(NX):
            copy(k).start()
        lhs = []
        for s in range(4):
            at = (place_ref[1] ^ s) * quarter
            parts = [lhs_ref[pl.ds(h * rows + at, quarter)] for h in range(heads)]
            lhs.append(jnp.concatenate(parts, axis=1))
        lhs = jnp.concatenate(lhs, axis=0)
        for k in range(NX):
            copy(k).wait()
            out_ref[k] = dot(lhs, w[k]).astype(out_ref.dtype)

    return pl.pallas_call(
        body,
        out_shape=pltpu.VMEM((NX, rows, block), BF16 if give else F32),
        in_specs=[SMEM, VMEM, HBM],
        out_specs=VMEM,
        scratch_shapes=[
            pltpu.VMEM((NX, depth, block), BF16),
            pltpu.SemaphoreType.DMA((NX,)),
        ],
        name="out_give" if give else "out_keep",
    )(place, *in_vmem(attended), w_out)


def hidden_terms(place, gains, pieces, weights, first):
    n, part, depth = pieces[0].shape
    rows, cols, count = 4 * part, weights[0].shape[1], len(pieces)

    def body(place_ref, gain_ref, *refs):
        pieces, weights, refs = refs[:count], refs[count : count + n], refs[count + n :]
        give_ref, keep_ref = refs[:2]
        w, acc, sq, sem = refs[-4:]
        copies = [
            pltpu.make_async_copy(weights[k], w.at[k], sem.at[k]) for k in range(n)
        ]
        for copy in copies:
            copy.start()
        for k in range(n):
            wide = jnp.concatenate([p[k] for p in pieces], axis=0).astype(F32)
            gain = gain_ref[place_ref[3] * n + (place_ref[2] + k) % n]
            lhs = (wide * gain).astype(BF16)
            copies[k].wait()
            out = dot(lhs, w[k])
            acc[...] = out if k == 0 else acc[...] + out
            if first:
                square = jnp.sum(wide * wide, axis=1, keepdims=True)
                square = jnp.broadcast_to(square, sq.shape)
                sq[...] = square if k == 0 else sq[...] + square
        keep = pl.multiple_of((place_ref[3] ^ place_ref[0]) * rows, rows)
        give = pl.multiple_of(((1 - place_ref[3]) ^ place_ref[0]) * rows, rows)
        give_ref[:, :cols] = acc[pl.ds(give, rows)].astype(BF16)
        keep_ref[...] = acc[pl.ds(keep, rows)]
        if first:
            square = sq[pl.ds(give, rows)]
            top = square.astype(BF16).astype(F32)
            lane = lax.broadcasted_iota(jnp.int32, square.shape, 1)
            give_ref[:, cols:] = jnp.where(lane == 0, top, square - top).astype(BF16)
            refs[2][...] = sq[pl.ds(keep, rows)]

    keeps = [(rows, cols), (rows, 128)][: 2 if first else 1]
    return pl.pallas_call(
        body,
        out_shape=[pltpu.VMEM((rows, cols + (128 if first else 0)), BF16)]
        + [jax.ShapeDtypeStruct(shape, F32) for shape in keeps],
        in_specs=[SMEM, VMEM] + [VMEM] * count + [HBM] * n,
        out_specs=[VMEM] * (1 + len(keeps)),
        scratch_shapes=[
            pltpu.VMEM((n, depth, cols), BF16),
            pltpu.VMEM((2 * rows, cols), F32),
            pltpu.VMEM((2 * rows, 128), F32),
            pltpu.SemaphoreType.DMA((n,)),
        ],
        name="gate" if first else "up",
    )(place, gains, *in_vmem(*pieces), *weights)


def hidden_units(gate, up, square, sent_gate, sent_up, dim):
    rows, cols = gate.shape

    def body(gate_ref, up_ref, square_ref, sent_gate_ref, sent_up_ref, out_ref):
        extra = sent_gate_ref[:, cols:].astype(F32)
        mean = (square_ref[:, :1] + extra[:, :1] + extra[:, 1:2]) / dim
        factor = lax.rsqrt(mean + EPS)
        gate = (gate_ref[...] + sent_gate_ref[:, :cols].astype(F32)) * factor
        up = (up_ref[...] + sent_up_ref[...].astype(F32)) * factor
        out_ref[...] = (gate / (1.0 + jnp.exp(-gate)) * up).astype(BF16)

    return pl.pallas_call(
        body,
        out_shape=pltpu.VMEM((rows, cols), BF16),
        in_specs=[VMEM] * 5,
        out_specs=VMEM,
        name="hidden",
    )(gate, up, square, *in_vmem(sent_gate, sent_up))


def down_terms(place, hidden, other, weights, give):
    n, rows = len(weights), hidden.shape[0]
    depth, cols = weights[0].shape

    def body(place_ref, hidden_ref, other_ref, *refs):
        weights, out_ref, w, sem = refs[:n], refs[n], refs[n + 1], refs[n + 2]
        copies = [
            pltpu.make_async_copy(weights[k], w.at[k], sem.at[k]) for k in range(n)
        ]
        for copy in copies:
            copy.start()
        same = place_ref[0] == place_ref[3]
        own = jnp.logical_not(same) if give else same
        lhs = jnp.where(own, hidden_ref[...], other_ref[...])
        for k in range(n):
            copies[k].wait()
            out_ref[k] = dot(lhs, w[k]).astype(out_ref.dtype)

    return pl.pallas_call(
        body,
        out_shape=pltpu.VMEM((n, rows, cols), BF16 if give else F32),
        in_specs=[SMEM, VMEM, VMEM] + [HBM] * n,
        out_specs=VMEM,
        scratch_shapes=[pltpu.VMEM((n, depth, cols), BF16), pltpu.SemaphoreType.DMA((n,))],
        name="down_give" if give else "down_keep",
    )(place, *in_vmem(hidden, other), *weights)


def rope_tables(positions):
    half = HD // 2
    frequency = THETA ** (-jnp.arange(half, dtype=F32) * 2.0 / HD)
    angles = positions.astype(F32)[:, None] * frequency[None, :]
    return jnp.cos(angles), jnp.sin(angles)


def pick(array, index, axis=0):
    return lax.dynamic_index_in_dim(array, index, axis, keepdims=False)


def from_x(array, r):
    return lax.ppermute(array, "x", [(i, (i - r) % NX) for i in range(NX)])


def project(place, pieces, gains, w_query, w_keyval, mode, sums=()):
    arrays = [piece for piece, _, _ in pieces]
    n_z, rows, width = arrays[0].shape
    n_q, n_kv = w_query.shape[1], w_keyval.shape[0]
    steps = n_z * len(arrays)
    do_q, do_kv = mode != "kv", mode != "q"

    def body(place_ref, gain_ref, wq_hbm, wkv_hbm, *refs):
        refs, rest = refs[: len(arrays)], refs[len(arrays) :]
        before, rest = rest[: len(sums)], rest[len(sums) :]
        if mode == "first":
            q_ref, kv_ref, sq_ref = rest[:3]
        elif mode == "kv":
            (kv_ref, factor_ref), sq_ref = rest[:2], rest[2]
        else:
            q_ref = rest[0]
        wq, wkv, sem_q, sem_kv = rest[-4:]

        def at(i):
            _, s, rc = pieces[i // n_z]
            return ((place_ref[0] ^ rc) * n_z + i % n_z) * 4 + (place_ref[1] ^ s)

        def copies(i):
            g, out = at(i) * width, []
            if do_q:
                rows_q = wq_hbm.at[pl.ds(g, width)]
                out.append(pltpu.make_async_copy(rows_q, wq.at[i], sem_q.at[i]))
            if do_kv:
                cols_kv = wkv_hbm.at[:, pl.ds(g, width)]
                out.append(pltpu.make_async_copy(cols_kv, wkv.at[i], sem_kv.at[i]))
            return out

        for i in range(steps):
            for copy in copies(i):
                copy.start()
        if mode == "first":
            for ref in (q_ref, kv_ref, sq_ref):
                ref[...] = jnp.zeros(ref.shape, F32)
        elif mode == "kv":
            kv_ref[...], sq_ref[...] = before[0][...], before[1][...]
        else:
            q_ref[...] = before[0][...]
        for p, ref in enumerate(refs):
            q = q_ref[...] if do_q else None
            kv = kv_ref[...] if do_kv else None
            for r in range(n_z):
                i = p * n_z + r
                piece = ref[r].astype(F32)
                lhs = (piece * gain_ref[at(i)]).astype(BF16)
                for copy in copies(i):
                    copy.wait()
                if do_q:
                    q = q + dot(lhs, wq[i])
                if do_kv:
                    sq_ref[...] += piece * piece
                    kv = kv + dot_t(wkv[i], lhs)
            if do_q:
                q_ref[...] = q
            if do_kv:
                kv_ref[...] = kv
        if mode == "kv":
            mean = jnp.sum(sq_ref[...], axis=1, keepdims=True) / (32 * width)
            factor = jnp.broadcast_to(lax.rsqrt(mean + EPS), (rows, rows))
            factor_ref[...] = factor
            kv_ref[...] = kv_ref[...] * factor.T[:1]
        elif mode == "q":
            q_ref[...] = q_ref[...] * before[1][:, :1]

    shapes = {
        "first": [(rows, n_q), (n_kv, rows), (rows, width)],
        "kv": [(n_kv, rows), (rows, rows)],
        "q": [(rows, n_q)],
    }[mode]
    return pl.pallas_call(
        body,
        out_shape=[pltpu.VMEM(shape, F32) for shape in shapes],
        in_specs=[SMEM, VMEM, HBM, HBM] + [VMEM] * (len(arrays) + len(sums)),
        out_specs=[VMEM] * len(shapes),
        scratch_shapes=([pltpu.VMEM((rows, width), F32)] if mode == "kv" else [])
        + [
            pltpu.VMEM((steps if do_q else 1, width, n_q), BF16),
            pltpu.VMEM((steps if do_kv else 1, n_kv, width), BF16),
            pltpu.SemaphoreType.DMA((steps,)),
            pltpu.SemaphoreType.DMA((steps,)),
        ],
    )(place, *in_vmem(gains), w_query, w_keyval, *in_vmem(*arrays, *sums))


def over_square(terms, sent):
    quarter = terms.shape[1] // 4

    def both(s):
        rows = slice(s * quarter, (s + 1) * quarter)
        return terms[:, rows] + sent[:, rows].astype(F32)

    got = [from_sq(both(s).astype(BF16), s) for s in (1, 2, 3)]
    return (both(0) + sum(t.astype(F32) for t in got)).astype(BF16)


def gathered(piece):
    near = to_all(piece, "zh")
    ours = [near] + [from_sq(near, s) for s in (1, 2, 3)]
    theirs = [lax.ppermute(t, "c", SWAP) for t in ours]
    return ours, theirs


def layer(tokens_in, gain_attn, w_query, w_keyval, w_out, gain_mlp, w_gate, w_up, w_down):
    core, y_hi, x = lax.axis_index("c"), lax.axis_index("yh"), lax.axis_index("x")
    z_hi, z_lo, y_lo = lax.axis_index("zh"), lax.axis_index("zl"), lax.axis_index("yl")
    block, spot = lax.axis_index(DP), z_lo * 2 + y_lo
    rows, width = tokens_in.shape
    n_dp, n_z = lax.axis_size(DP), lax.axis_size(Z)
    dim = w_query.shape[0]
    block_d = dim // 8
    total = rows * n_dp
    quarter = rows // 4

    gate_next, gate_last = from_x(w_gate, 1), from_x(w_gate, 3)
    up_next, up_last = from_x(w_up, 1), from_x(w_up, 3)
    gate_all = [w_gate, gate_next, from_x(gate_next, 1), gate_last]
    up_all = [w_up, up_next, from_x(up_last, 3), up_last]
    down_next, down_last = from_x(w_down, 1), from_x(w_down, 3)
    down_all = [w_down, down_next, from_x(down_next, 1), down_last]

    ours, theirs = gathered(tokens_in)
    place = jnp.stack([core, spot, x, y_hi]).astype(jnp.int32)
    gains = gain_attn.astype(F32).reshape(4 * n_z, 1, width)
    pieces = [(t, s, rc) for rc, side in ((0, ours), (1, theirs)) for s, t in enumerate(side)]
    early = [p for p in pieces if p[1] == 0]
    late = [p for p in pieces if p[1] != 0]
    w_kv = w_keyval.T
    q_sum, kv_sum, squares = project(place, early, gains, w_query, w_kv, "first")
    kv_part, factor = project(place, late, gains, w_query, w_kv, "kv", (kv_sum, squares))
    (query,) = project(place, late, gains, w_query, w_kv, "q", (q_sum, factor))

    kv_here = move(
        kv_part.astype(BF16),
        lambda c, zh, zl, **_: {"c": zh // 2, "zh": (zh % 2) * 2 + zl, "zl": c},
    )
    parts = to_all(kv_here, ("yh", "x", "zl", "yl")).reshape(n_dp, 2, HD, rows)
    key_t = jnp.moveaxis(parts[:, 0], 0, 1).reshape(HD, total)
    value_t = jnp.moveaxis(parts[:, 1], 0, 1).reshape(HD, total)

    key_pos = jnp.arange(total, dtype=jnp.int32)
    cos_k, sin_k = rope_tables(key_pos)
    cos_k, sin_k = cos_k.T, sin_k.T
    k1, k2 = key_t[: HD // 2].astype(F32), key_t[HD // 2 :].astype(F32)
    key_rot = jnp.concatenate(
        [k1 * cos_k - k2 * sin_k, k2 * cos_k + k1 * sin_k], axis=0
    ).astype(BF16)
    pos = block * rows + jnp.arange(rows, dtype=jnp.int32)
    cos_q, sin_q = rope_tables(pos)
    heads = w_query.shape[1] // HD
    q_rot = []
    for h in range(heads):
        q1 = query[:, h * HD : h * HD + HD // 2]
        q2 = query[:, h * HD + HD // 2 : (h + 1) * HD]
        q_rot.append(jnp.concatenate([q1 * cos_q - q2 * sin_q, q2 * cos_q + q1 * sin_q], axis=1))
    q_rot = jnp.concatenate(q_rot, axis=0).astype(BF16)
    scores = dot(q_rot, key_rot) * HD ** (-0.5)
    allowed = key_pos[None, :] <= jnp.tile(pos, heads)[:, None]
    scores = jnp.where(allowed, scores, -1e30)
    expo = jnp.exp(scores - jnp.max(scores, axis=-1, keepdims=True))
    probs = (expo / jnp.sum(expo, axis=-1, keepdims=True)).astype(BF16)
    attended = lax.dot_general(
        probs, value_t, (((1,), (1,)), ((), ())), preferred_element_type=F32
    ).astype(BF16)
    sent = lax.ppermute(out_terms(place, attended, w_out, True), "c", SWAP)
    terms = out_terms(place, attended, w_out, False)
    resid = [
        lax.dynamic_slice(t, ((x + z_hi) % NX, spot * quarter, 0), (1, quarter, width))[0]
        for t in ours
    ]
    resid = jnp.stack(resid, axis=0)
    resid = jnp.concatenate([pick(resid, j ^ spot) for j in range(4)], axis=1)
    tiles = over_square(terms, sent)
    tiles = exchange(tiles, "zh")
    mid_part = (resid.astype(F32) + tiles.astype(F32).sum(axis=0)).astype(BF16)
    mid_own = move(mid_part, lambda c, yh, **_: {"c": yh, "yh": c})

    ours, theirs = gathered(mid_own)

    gains_mlp = gain_mlp.astype(F32).reshape(n_dp, 1, block_d)
    mids = ours + theirs
    sent, gate, square = hidden_terms(place, gains_mlp, mids, gate_all, True)
    sent_gate = lax.ppermute(sent, "yh", SWAP)
    sent, up = hidden_terms(place, gains_mlp, mids, up_all, False)
    sent_up = lax.ppermute(sent, "yh", SWAP)
    hidden = hidden_units(gate, up, square, sent_gate, sent_up, dim)

    other = lax.ppermute(hidden, "yh", SWAP)
    sent = down_terms(place, hidden, other, down_all, True)
    sent = lax.ppermute(sent, "c", SWAP)
    terms = down_terms(place, hidden, other, down_all, False)
    tiles = exchange(over_square(terms, sent), "zh")
    done = (mid_own.astype(F32) + tiles.astype(F32).sum(axis=0)).astype(BF16)
    return move(done, lambda x, zh, **_: {"x": (x + zh) % NX, "zh": x})


def solution(mesh):
    fine = Mesh(mesh.devices.reshape(SIZES), EVERY)
    placed = (
        P(DP, GROUP),
        P(),
        P(None, GROUP),
        P(None, GROUP),
        P(GROUP, None),
        P(),
        P(DP, GROUP),
        P(DP, GROUP),
        P(GROUP, DP),
    )
    return jax.shard_map(layer, mesh=fine, in_specs=placed, out_specs=P(GROUP, DP), check_vma=False)
```

```python
import jax
import jax.numpy as jnp
from jax import lax
from jax.experimental import pallas as pl
from jax.experimental.pallas import tpu as pltpu
from jax.sharding import Mesh
from jax.sharding import PartitionSpec as P


HD = 128
EPS = 1e-05
THETA = 10000.0

F32 = jnp.float32
BF16 = jnp.bfloat16
DP = ("yh", "x")
Z = ("zh", "zl")
GROUP = ("c", "zh", "zl", "yl")
EVERY = ("c", "yh", "x", "zh", "zl", "yl")
SIZES = (2, 2, 4, 4, 2, 2)
SWAP = [(0, 1), (1, 0)]
NX = 4


def dot(a, b):
    return jnp.dot(a, b, preferred_element_type=F32)


def dot_t(a, b):
    return lax.dot_general(a, b, (((1,), (1,)), ((), ())), preferred_element_type=F32)


def to_all(array, axis):
    length = lax.axis_size(axis)
    return exchange(jnp.broadcast_to(array[None], (length, *array.shape)), axis)


def exchange(tiles, axis):
    return lax.all_to_all(tiles, axis, 0, 0, tiled=True)


def from_sq(array, s):
    return lax.ppermute(array, ("zl", "yl"), [(i, i ^ s) for i in range(4)])


def move(array, target):
    moves = []
    for n in range(256):
        at, rest = {}, n
        for name, size in zip(reversed(EVERY), reversed(SIZES)):
            at[name] = rest % size
            rest //= size
        goal, to = {**at, **target(**at)}, 0
        for name, size in zip(EVERY, SIZES):
            to = to * size + goal[name]
        moves.append((n, to))
    return lax.ppermute(array, EVERY, moves)


VMEM = pl.BlockSpec(memory_space=pltpu.VMEM)
SMEM = pl.BlockSpec(memory_space=pltpu.SMEM)
HBM = pl.BlockSpec(memory_space=pl.ANY)


def in_vmem(*arrays):
    return [pltpu.with_memory_space_constraint(t, pltpu.VMEM) for t in arrays]


def out_terms(place, attended, w_out, give):
    depth, block = w_out.shape[0], w_out.shape[1] // (2 * NX)
    heads = depth // HD
    rows = attended.shape[0] // heads
    quarter = rows // 4

    def body(place_ref, lhs_ref, w_hbm, out_ref, w, sem):
        half = 1 - place_ref[0] if give else place_ref[0]

        def copy(k):
            at = (half * NX + (place_ref[2] + k) % NX) * block
            return pltpu.make_async_copy(w_hbm.at[:, pl.ds(at, block)], w.at[k], sem.at[k])

        for k in range(NX):
            copy(k).start()
        lhs = []
        for s in range(4):
            at = (place_ref[1] ^ s) * quarter
            parts = [lhs_ref[pl.ds(h * rows + at, quarter)] for h in range(heads)]
            lhs.append(jnp.concatenate(parts, axis=1))
        lhs = jnp.concatenate(lhs, axis=0)
        for k in range(NX):
            copy(k).wait()
            out_ref[k] = dot(lhs, w[k]).astype(out_ref.dtype)

    return pl.pallas_call(
        body,
        out_shape=pltpu.VMEM((NX, rows, block), BF16 if give else F32),
        in_specs=[SMEM, VMEM, HBM],
        out_specs=VMEM,
        scratch_shapes=[
            pltpu.VMEM((NX, depth, block), BF16),
            pltpu.SemaphoreType.DMA((NX,)),
        ],
        name="out_give" if give else "out_keep",
    )(place, *in_vmem(attended), w_out)


def gate_up_terms(place, gains, pieces, gates, ups):
    n, part, depth = pieces[0].shape
    rows, hid, count = 4 * part, gates[0].shape[1], len(pieces)
    cols = 2 * hid

    def body(place_ref, gain_ref, *refs):
        pieces, refs = refs[:count], refs[count:]
        gates, ups, refs = refs[:n], refs[n : 2 * n], refs[2 * n :]
        give_ref, keep_ref, square_ref, w, acc, sq, sem = refs
        copies = [
            (
                pltpu.make_async_copy(gates[k], w.at[k, :, pl.ds(0, hid)], sem.at[2 * k]),
                pltpu.make_async_copy(ups[k], w.at[k, :, pl.ds(hid, hid)], sem.at[2 * k + 1]),
            )
            for k in range(n)
        ]
        for pair in copies:
            for copy in pair:
                copy.start()
        for k in range(n):
            lhs = jnp.concatenate([p[k] for p in pieces], axis=0)
            wide = lhs.astype(F32)
            square = jnp.sum(wide * wide, axis=1, keepdims=True)
            for copy in copies[k]:
                copy.wait()
            gain = gain_ref[place_ref[3] * n + (place_ref[2] + k) % n]
            out = dot((wide * gain).astype(BF16), w[k])
            if k == 0:
                acc[...], sq[...] = out, jnp.broadcast_to(square, sq.shape)
            else:
                acc[...] += out
                sq[...] += square
        keep = pl.multiple_of((place_ref[3] ^ place_ref[0]) * rows, rows)
        give = pl.multiple_of(((1 - place_ref[3]) ^ place_ref[0]) * rows, rows)
        give_ref[:, :cols] = acc[pl.ds(give, rows)].astype(BF16)
        square = sq[pl.ds(give, rows)]
        top = square.astype(BF16)
        low = (square - top.astype(F32)).astype(BF16)
        lane = lax.broadcasted_iota(jnp.int32, square.shape, 1)
        give_ref[:, cols:] = jnp.where(lane == 0, top.astype(F32), low.astype(F32)).astype(BF16)
        keep_ref[...] = acc[pl.ds(keep, rows)]
        square_ref[...] = sq[pl.ds(keep, rows)]

    return pl.pallas_call(
        body,
        out_shape=[
            pltpu.VMEM((rows, cols + 128), BF16),
            jax.ShapeDtypeStruct((rows, cols), F32),
            jax.ShapeDtypeStruct((rows, 128), F32),
        ],
        in_specs=[SMEM, VMEM] + [VMEM] * count + [HBM] * (2 * n),
        out_specs=[VMEM] * 3,
        scratch_shapes=[
            pltpu.VMEM((n, depth, cols), BF16),
            pltpu.VMEM((2 * rows, cols), F32),
            pltpu.VMEM((2 * rows, 128), F32),
            pltpu.SemaphoreType.DMA((2 * n,)),
        ],
        name="gate_up",
    )(place, gains, *in_vmem(*pieces), *gates, *ups)


def hidden_units(keep, square, sent, dim):
    rows, cols = keep.shape

    def body(keep_ref, square_ref, sent_ref, out_ref):
        extra = sent_ref[:, cols:].astype(F32)
        mean = (square_ref[:, :1] + extra[:, :1] + extra[:, 1:2]) / dim
        out = (keep_ref[...] + sent_ref[:, :cols].astype(F32)) * lax.rsqrt(mean + EPS)
        gate, up = out[:, : cols // 2], out[:, cols // 2 :]
        out_ref[...] = (gate / (1.0 + jnp.exp(-gate)) * up).astype(BF16)

    return pl.pallas_call(
        body,
        out_shape=pltpu.VMEM((rows, cols // 2), BF16),
        in_specs=[VMEM] * 3,
        out_specs=VMEM,
        name="hidden",
    )(keep, square, *in_vmem(sent))


def down_terms(place, hidden, other, weights, give):
    n, rows = len(weights), hidden.shape[0]
    depth, cols = weights[0].shape

    def body(place_ref, hidden_ref, other_ref, *refs):
        weights, out_ref, w, sem = refs[:n], refs[n], refs[n + 1], refs[n + 2]
        copies = [
            pltpu.make_async_copy(weights[k], w.at[k], sem.at[k]) for k in range(n)
        ]
        for copy in copies:
            copy.start()
        same = place_ref[0] == place_ref[3]
        own = jnp.logical_not(same) if give else same
        lhs = jnp.where(own, hidden_ref[...], other_ref[...])
        for k in range(n):
            copies[k].wait()
            out_ref[k] = dot(lhs, w[k]).astype(out_ref.dtype)

    return pl.pallas_call(
        body,
        out_shape=pltpu.VMEM((n, rows, cols), BF16 if give else F32),
        in_specs=[SMEM, VMEM, VMEM] + [HBM] * n,
        out_specs=VMEM,
        scratch_shapes=[pltpu.VMEM((n, depth, cols), BF16), pltpu.SemaphoreType.DMA((n,))],
        name="down_give" if give else "down_keep",
    )(place, *in_vmem(hidden, other), *weights)


def rope_tables(positions):
    half = HD // 2
    frequency = THETA ** (-jnp.arange(half, dtype=F32) * 2.0 / HD)
    angles = positions.astype(F32)[:, None] * frequency[None, :]
    return jnp.cos(angles), jnp.sin(angles)


def pick(array, index, axis=0):
    return lax.dynamic_index_in_dim(array, index, axis, keepdims=False)


def from_x(array, r):
    return lax.ppermute(array, "x", [(i, (i - r) % NX) for i in range(NX)])


def project(place, pieces, gains, w_query, w_keyval, sums):
    arrays = [piece for piece, _, _ in pieces]
    n_z, rows, width = arrays[0].shape
    n_q, n_kv = w_query.shape[1], w_keyval.shape[0]
    steps = n_z * len(arrays)
    last = sums is not None

    def body(place_ref, gain_ref, wq_hbm, wkv_hbm, *refs):
        refs, rest = refs[: len(arrays)], refs[len(arrays) :]
        before, rest = (rest[:3], rest[3:]) if last else (None, rest)
        q_ref, kv_ref, sq_ref, wq, wkv, sem_q, sem_kv = rest

        def at(i):
            _, s, rc = pieces[i // n_z]
            return ((place_ref[0] ^ rc) * n_z + i % n_z) * 4 + (place_ref[1] ^ s)

        def copies(i):
            g = at(i) * width
            return (
                pltpu.make_async_copy(wq_hbm.at[pl.ds(g, width)], wq.at[i], sem_q.at[i]),
                pltpu.make_async_copy(wkv_hbm.at[:, pl.ds(g, width)], wkv.at[i], sem_kv.at[i]),
            )

        for i in range(steps):
            for copy in copies(i):
                copy.start()
        if last:
            for ref, old in zip((q_ref, kv_ref, sq_ref), before):
                ref[...] = old[...]
        else:
            for ref in (q_ref, kv_ref, sq_ref):
                ref[...] = jnp.zeros(ref.shape, F32)
        for p, ref in enumerate(refs):
            q, kv = q_ref[...], kv_ref[...]
            for r in range(n_z):
                i = p * n_z + r
                piece = ref[r].astype(F32)
                lhs = (piece * gain_ref[at(i)]).astype(BF16)
                sq_ref[...] += piece * piece
                for copy in copies(i):
                    copy.wait()
                q, kv = q + dot(lhs, wq[i]), kv + dot_t(wkv[i], lhs)
            q_ref[...], kv_ref[...] = q, kv
        if last:
            mean = jnp.sum(sq_ref[...], axis=1, keepdims=True) / (32 * width)
            factor = lax.rsqrt(mean + EPS)
            q_ref[...] = q_ref[...] * factor
            across = jnp.broadcast_to(factor, (rows, rows)).T[:1]
            kv_ref[...] = kv_ref[...] * across

    shapes = [(rows, n_q), (n_kv, rows), (rows, width)]
    return pl.pallas_call(
        body,
        out_shape=[pltpu.VMEM(shape, F32) for shape in shapes],
        in_specs=[SMEM, VMEM, HBM, HBM] + [VMEM] * (len(arrays) + (3 if last else 0)),
        out_specs=[VMEM] * 3,
        scratch_shapes=[
            pltpu.VMEM((steps, width, n_q), BF16),
            pltpu.VMEM((steps, n_kv, width), BF16),
            pltpu.SemaphoreType.DMA((steps,)),
            pltpu.SemaphoreType.DMA((steps,)),
        ],
        name="project_last" if last else "project_first",
    )(place, *in_vmem(gains), w_query, w_keyval, *in_vmem(*arrays, *(sums or ())))


def over_square(terms, sent):
    quarter = terms.shape[1] // 4

    def both(s):
        rows = slice(s * quarter, (s + 1) * quarter)
        return terms[:, rows] + sent[:, rows].astype(F32)

    got = [from_sq(both(s).astype(BF16), s) for s in (1, 2, 3)]
    return (both(0) + sum(t.astype(F32) for t in got)).astype(BF16)


def gathered(piece):
    near = to_all(piece, "zh")
    ours = [near] + [from_sq(near, s) for s in (1, 2, 3)]
    theirs = [lax.ppermute(t, "c", SWAP) for t in ours]
    return ours, theirs


def layer(tokens_in, gain_attn, w_query, w_keyval, w_out, gain_mlp, w_gate, w_up, w_down):
    core, y_hi, x = lax.axis_index("c"), lax.axis_index("yh"), lax.axis_index("x")
    z_hi, z_lo, y_lo = lax.axis_index("zh"), lax.axis_index("zl"), lax.axis_index("yl")
    block, spot = lax.axis_index(DP), z_lo * 2 + y_lo
    rows, width = tokens_in.shape
    n_dp, n_z = lax.axis_size(DP), lax.axis_size(Z)
    dim = w_query.shape[0]
    block_d = dim // 8
    total = rows * n_dp
    quarter = rows // 4

    gate_next, gate_last = from_x(w_gate, 1), from_x(w_gate, 3)
    up_next, up_last = from_x(w_up, 1), from_x(w_up, 3)
    gate_all = [w_gate, gate_next, from_x(gate_next, 1), gate_last]
    up_all = [w_up, up_next, from_x(up_last, 3), up_last]
    down_next, down_last = from_x(w_down, 1), from_x(w_down, 3)
    down_all = [w_down, down_next, from_x(down_next, 1), down_last]

    ours, theirs = gathered(tokens_in)
    place = jnp.stack([core, spot, x, y_hi]).astype(jnp.int32)
    gains = gain_attn.astype(F32).reshape(4 * n_z, 1, width)
    pieces = [(t, s, rc) for rc, side in ((0, ours), (1, theirs)) for s, t in enumerate(side)]
    early = [p for p in pieces if p[1] == 0]
    late = [p for p in pieces if p[1] != 0]
    w_kv = w_keyval.T
    sums = project(place, early, gains, w_query, w_kv, None)
    query, kv_part, _ = project(place, late, gains, w_query, w_kv, sums)

    kv_here = move(
        kv_part.astype(BF16),
        lambda c, zh, zl, **_: {"c": zh // 2, "zh": (zh % 2) * 2 + zl, "zl": c},
    )
    parts = to_all(kv_here, ("yh", "x", "zl", "yl")).reshape(n_dp, 2, HD, rows)
    key_t = jnp.moveaxis(parts[:, 0], 0, 1).reshape(HD, total)
    value_t = jnp.moveaxis(parts[:, 1], 0, 1).reshape(HD, total)

    key_pos = jnp.arange(total, dtype=jnp.int32)
    cos_k, sin_k = rope_tables(key_pos)
    cos_k, sin_k = cos_k.T, sin_k.T
    k1, k2 = key_t[: HD // 2].astype(F32), key_t[HD // 2 :].astype(F32)
    key_rot = jnp.concatenate(
        [k1 * cos_k - k2 * sin_k, k2 * cos_k + k1 * sin_k], axis=0
    ).astype(BF16)
    pos = block * rows + jnp.arange(rows, dtype=jnp.int32)
    cos_q, sin_q = rope_tables(pos)
    heads = w_query.shape[1] // HD
    q_rot = []
    for h in range(heads):
        q1 = query[:, h * HD : h * HD + HD // 2]
        q2 = query[:, h * HD + HD // 2 : (h + 1) * HD]
        q_rot.append(jnp.concatenate([q1 * cos_q - q2 * sin_q, q2 * cos_q + q1 * sin_q], axis=1))
    q_rot = jnp.concatenate(q_rot, axis=0).astype(BF16)
    scores = dot(q_rot, key_rot) * HD ** (-0.5)
    allowed = key_pos[None, :] <= jnp.tile(pos, heads)[:, None]
    scores = jnp.where(allowed, scores, -1e30)
    expo = jnp.exp(scores - jnp.max(scores, axis=-1, keepdims=True))
    probs = (expo / jnp.sum(expo, axis=-1, keepdims=True)).astype(BF16)
    attended = lax.dot_general(
        probs, value_t, (((1,), (1,)), ((), ())), preferred_element_type=F32
    ).astype(BF16)
    sent = lax.ppermute(out_terms(place, attended, w_out, True), "c", SWAP)
    terms = out_terms(place, attended, w_out, False)
    resid = [
        lax.dynamic_slice(t, ((x + z_hi) % NX, spot * quarter, 0), (1, quarter, width))[0]
        for t in ours
    ]
    resid = jnp.stack(resid, axis=0)
    resid = jnp.concatenate([pick(resid, j ^ spot) for j in range(4)], axis=1)
    tiles = over_square(terms, sent)
    tiles = exchange(tiles, "zh")
    mid_part = (resid.astype(F32) + tiles.astype(F32).sum(axis=0)).astype(BF16)
    mid_own = move(mid_part, lambda c, yh, **_: {"c": yh, "yh": c})

    ours, theirs = gathered(mid_own)

    gains_mlp = gain_mlp.astype(F32).reshape(n_dp, 1, block_d)
    sent, keep, square = gate_up_terms(place, gains_mlp, ours + theirs, gate_all, up_all)
    sent = lax.ppermute(sent, "yh", SWAP)
    hidden = hidden_units(keep, square, sent, dim)

    other = lax.ppermute(hidden, "yh", SWAP)
    sent = down_terms(place, hidden, other, down_all, True)
    sent = lax.ppermute(sent, "c", SWAP)
    terms = down_terms(place, hidden, other, down_all, False)
    tiles = exchange(over_square(terms, sent), "zh")
    done = (mid_own.astype(F32) + tiles.astype(F32).sum(axis=0)).astype(BF16)
    return move(done, lambda x, zh, **_: {"x": (x + zh) % NX, "zh": x})


def solution(mesh):
    fine = Mesh(mesh.devices.reshape(SIZES), EVERY)
    placed = (
        P(DP, GROUP),
        P(),
        P(None, GROUP),
        P(None, GROUP),
        P(GROUP, None),
        P(),
        P(DP, GROUP),
        P(DP, GROUP),
        P(GROUP, DP),
    )
    return jax.shard_map(layer, mesh=fine, in_specs=placed, out_specs=P(GROUP, DP), check_vma=False)
```

```python
import jax
import jax.numpy as jnp
from jax import lax
from jax.experimental import pallas as pl
from jax.experimental.pallas import tpu as pltpu
from jax.sharding import Mesh
from jax.sharding import PartitionSpec as P


HD = 128
EPS = 1e-05
THETA = 10000.0

F32 = jnp.float32
BF16 = jnp.bfloat16
DP = ("yh", "x")
Z = ("zh", "zl")
GROUP = ("c", "zh", "zl", "yl")
EVERY = ("c", "yh", "x", "zh", "zl", "yl")
SIZES = (2, 2, 4, 4, 2, 2)
SWAP = [(0, 1), (1, 0)]
NX = 4


def dot(a, b):
    return jnp.dot(a, b, preferred_element_type=F32)


def dot_t(a, b):
    return lax.dot_general(a, b, (((1,), (1,)), ((), ())), preferred_element_type=F32)


def to_all(array, axis):
    length = lax.axis_size(axis)
    return exchange(jnp.broadcast_to(array[None], (length, *array.shape)), axis)


def exchange(tiles, axis):
    return lax.all_to_all(tiles, axis, 0, 0, tiled=True)


def from_sq(array, s):
    return lax.ppermute(array, ("zl", "yl"), [(i, i ^ s) for i in range(4)])


def move(array, target):
    moves = []
    for n in range(256):
        at, rest = {}, n
        for name, size in zip(reversed(EVERY), reversed(SIZES)):
            at[name] = rest % size
            rest //= size
        goal, to = {**at, **target(**at)}, 0
        for name, size in zip(EVERY, SIZES):
            to = to * size + goal[name]
        moves.append((n, to))
    return lax.ppermute(array, EVERY, moves)


VMEM = pl.BlockSpec(memory_space=pltpu.VMEM)
SMEM = pl.BlockSpec(memory_space=pltpu.SMEM)
HBM = pl.BlockSpec(memory_space=pl.ANY)


def in_vmem(*arrays):
    return [pltpu.with_memory_space_constraint(t, pltpu.VMEM) for t in arrays]


def out_terms(place, attended, w_out, give):
    depth, block = w_out.shape[0], w_out.shape[1] // (2 * NX)
    heads = depth // HD
    rows = attended.shape[0] // heads
    quarter = rows // 4

    def body(place_ref, lhs_ref, w_hbm, out_ref, w, sem):
        half = 1 - place_ref[0] if give else place_ref[0]

        def copy(k):
            at = (half * NX + (place_ref[2] + k) % NX) * block
            return pltpu.make_async_copy(w_hbm.at[:, pl.ds(at, block)], w.at[k], sem.at[k])

        for k in range(NX):
            copy(k).start()
        lhs = []
        for s in range(4):
            at = (place_ref[1] ^ s) * quarter
            parts = [lhs_ref[pl.ds(h * rows + at, quarter)] for h in range(heads)]
            lhs.append(jnp.concatenate(parts, axis=1))
        lhs = jnp.concatenate(lhs, axis=0)
        for k in range(NX):
            copy(k).wait()
            out_ref[k] = dot(lhs, w[k]).astype(out_ref.dtype)

    return pl.pallas_call(
        body,
        out_shape=pltpu.VMEM((NX, rows, block), BF16 if give else F32),
        in_specs=[SMEM, VMEM, HBM],
        out_specs=VMEM,
        scratch_shapes=[
            pltpu.VMEM((NX, depth, block), BF16),
            pltpu.SemaphoreType.DMA((NX,)),
        ],
        name="out_give" if give else "out_keep",
    )(place, *in_vmem(attended), w_out)


def gate_up_terms(place, gains, pieces, gates, ups):
    n, part, depth = pieces[0].shape
    rows, hid, count = 4 * part, gates[0].shape[1], len(pieces)
    cols = 2 * hid

    def body(place_ref, gain_ref, *refs):
        pieces, refs = refs[:count], refs[count:]
        gates, ups, refs = refs[:n], refs[n : 2 * n], refs[2 * n :]
        give_ref, keep_ref, square_ref, w, acc, sq, sem = refs
        copies = [
            (
                pltpu.make_async_copy(gates[k], w.at[k, :, pl.ds(0, hid)], sem.at[2 * k]),
                pltpu.make_async_copy(ups[k], w.at[k, :, pl.ds(hid, hid)], sem.at[2 * k + 1]),
            )
            for k in range(n)
        ]
        for pair in copies:
            for copy in pair:
                copy.start()
        for k in range(n):
            lhs = jnp.concatenate([p[k] for p in pieces], axis=0)
            wide = lhs.astype(F32)
            square = jnp.sum(wide * wide, axis=1, keepdims=True)
            for copy in copies[k]:
                copy.wait()
            gain = gain_ref[place_ref[3] * n + (place_ref[2] + k) % n]
            out = dot((wide * gain).astype(BF16), w[k])
            if k == 0:
                acc[...], sq[...] = out, jnp.broadcast_to(square, sq.shape)
            else:
                acc[...] += out
                sq[...] += square
        keep = pl.multiple_of((place_ref[3] ^ place_ref[0]) * rows, rows)
        give = pl.multiple_of(((1 - place_ref[3]) ^ place_ref[0]) * rows, rows)
        give_ref[:, :cols] = acc[pl.ds(give, rows)].astype(BF16)
        square = sq[pl.ds(give, rows)]
        top = square.astype(BF16)
        low = (square - top.astype(F32)).astype(BF16)
        lane = lax.broadcasted_iota(jnp.int32, square.shape, 1)
        give_ref[:, cols:] = jnp.where(lane == 0, top.astype(F32), low.astype(F32)).astype(BF16)
        keep_ref[...] = acc[pl.ds(keep, rows)]
        square_ref[...] = sq[pl.ds(keep, rows)]

    return pl.pallas_call(
        body,
        out_shape=[
            pltpu.VMEM((rows, cols + 128), BF16),
            jax.ShapeDtypeStruct((rows, cols), F32),
            jax.ShapeDtypeStruct((rows, 128), F32),
        ],
        in_specs=[SMEM, VMEM] + [VMEM] * count + [HBM] * (2 * n),
        out_specs=[VMEM] * 3,
        scratch_shapes=[
            pltpu.VMEM((n, depth, cols), BF16),
            pltpu.VMEM((2 * rows, cols), F32),
            pltpu.VMEM((2 * rows, 128), F32),
            pltpu.SemaphoreType.DMA((2 * n,)),
        ],
        name="gate_up",
    )(place, gains, *in_vmem(*pieces), *gates, *ups)


def hidden_units(keep, square, sent, dim):
    rows, cols = keep.shape

    def body(keep_ref, square_ref, sent_ref, out_ref):
        extra = sent_ref[:, cols:].astype(F32)
        mean = (square_ref[:, :1] + extra[:, :1] + extra[:, 1:2]) / dim
        out = (keep_ref[...] + sent_ref[:, :cols].astype(F32)) * lax.rsqrt(mean + EPS)
        gate, up = out[:, : cols // 2], out[:, cols // 2 :]
        out_ref[...] = (gate / (1.0 + jnp.exp(-gate)) * up).astype(BF16)

    return pl.pallas_call(
        body,
        out_shape=pltpu.VMEM((rows, cols // 2), BF16),
        in_specs=[VMEM] * 3,
        out_specs=VMEM,
        name="hidden",
    )(keep, square, *in_vmem(sent))


def down_terms(place, hidden, other, weights, give):
    n, rows = len(weights), hidden.shape[0]
    depth, cols = weights[0].shape

    def body(place_ref, hidden_ref, other_ref, *refs):
        weights, out_ref, w, sem = refs[:n], refs[n], refs[n + 1], refs[n + 2]
        copies = [
            pltpu.make_async_copy(weights[k], w.at[k], sem.at[k]) for k in range(n)
        ]
        for copy in copies:
            copy.start()
        same = place_ref[0] == place_ref[3]
        own = jnp.logical_not(same) if give else same
        lhs = jnp.where(own, hidden_ref[...], other_ref[...])
        for k in range(n):
            copies[k].wait()
            out_ref[k] = dot(lhs, w[k]).astype(out_ref.dtype)

    return pl.pallas_call(
        body,
        out_shape=pltpu.VMEM((n, rows, cols), BF16 if give else F32),
        in_specs=[SMEM, VMEM, VMEM] + [HBM] * n,
        out_specs=VMEM,
        scratch_shapes=[pltpu.VMEM((n, depth, cols), BF16), pltpu.SemaphoreType.DMA((n,))],
        name="down_give" if give else "down_keep",
    )(place, *in_vmem(hidden, other), *weights)


def rope_tables(positions):
    half = HD // 2
    frequency = THETA ** (-jnp.arange(half, dtype=F32) * 2.0 / HD)
    angles = positions.astype(F32)[:, None] * frequency[None, :]
    return jnp.cos(angles), jnp.sin(angles)


def pick(array, index, axis=0):
    return lax.dynamic_index_in_dim(array, index, axis, keepdims=False)


def from_x(array, r):
    return lax.ppermute(array, "x", [(i, (i - r) % NX) for i in range(NX)])


def project(place, pieces, gains, w_query, w_keyval, sums, last=False):
    arrays = [piece for piece, _, _ in pieces]
    n_z, rows, width = arrays[0].shape
    n_q, n_kv = w_query.shape[1], w_keyval.shape[0]
    steps = n_z * len(arrays)
    more = sums is not None

    def body(place_ref, gain_ref, wq_hbm, wkv_hbm, *refs):
        refs, rest = refs[: len(arrays)], refs[len(arrays) :]
        before, rest = (rest[:3], rest[3:]) if more else (None, rest)
        q_ref, kv_ref, sq_ref, wq, wkv, sem_q, sem_kv = rest

        def at(i):
            _, s, rc = pieces[i // n_z]
            zh = (place_ref[4] + i % n_z) % n_z
            return ((place_ref[0] ^ rc) * n_z + zh) * 4 + (place_ref[1] ^ s)

        def copies(i):
            g = at(i) * width
            return (
                pltpu.make_async_copy(wq_hbm.at[pl.ds(g, width)], wq.at[i], sem_q.at[i]),
                pltpu.make_async_copy(wkv_hbm.at[:, pl.ds(g, width)], wkv.at[i], sem_kv.at[i]),
            )

        for i in range(steps):
            for copy in copies(i):
                copy.start()
        if more:
            for ref, old in zip((q_ref, kv_ref, sq_ref), before):
                ref[...] = old[...]
        else:
            for ref in (q_ref, kv_ref, sq_ref):
                ref[...] = jnp.zeros(ref.shape, F32)
        for p, ref in enumerate(refs):
            q, kv = q_ref[...], kv_ref[...]
            for r in range(n_z):
                i = p * n_z + r
                piece = ref[r].astype(F32)
                lhs = (piece * gain_ref[at(i)]).astype(BF16)
                sq_ref[...] += piece * piece
                for copy in copies(i):
                    copy.wait()
                q, kv = q + dot(lhs, wq[i]), kv + dot_t(wkv[i], lhs)
            q_ref[...], kv_ref[...] = q, kv
        if last:
            mean = jnp.sum(sq_ref[...], axis=1, keepdims=True) / (32 * width)
            factor = lax.rsqrt(mean + EPS)
            q_ref[...] = q_ref[...] * factor
            across = jnp.broadcast_to(factor, (rows, rows)).T[:1]
            kv_ref[...] = kv_ref[...] * across

    shapes = [(rows, n_q), (n_kv, rows), (rows, width)]
    return pl.pallas_call(
        body,
        out_shape=[pltpu.VMEM(shape, F32) for shape in shapes],
        in_specs=[SMEM, VMEM, HBM, HBM] + [VMEM] * (len(arrays) + (3 if more else 0)),
        out_specs=[VMEM] * 3,
        scratch_shapes=[
            pltpu.VMEM((steps, width, n_q), BF16),
            pltpu.VMEM((steps, n_kv, width), BF16),
            pltpu.SemaphoreType.DMA((steps,)),
            pltpu.SemaphoreType.DMA((steps,)),
        ],
        name="project_last" if last else "project_next" if more else "project_first",
    )(place, *in_vmem(gains), w_query, w_keyval, *in_vmem(*arrays, *(sums or ())))


def over_square(terms, sent):
    quarter = terms.shape[1] // 4

    def both(s):
        rows = slice(s * quarter, (s + 1) * quarter)
        return terms[:, rows] + sent[:, rows].astype(F32)

    got = [from_sq(both(s).astype(BF16), s) for s in (1, 2, 3)]
    return (both(0) + sum(t.astype(F32) for t in got)).astype(BF16)


def gathered(piece, relative=False):
    if relative:
        near = [piece]
        for r in range(1, NX):
            hop = [(i, (i - r) % NX) for i in range(NX)]
            near.append(lax.ppermute(piece, "zh", hop))
        near = jnp.stack(near, axis=0)
    else:
        near = to_all(piece, "zh")
    ours = [near] + [from_sq(near, s) for s in (1, 2)]
    ours.append(from_sq(near, 3))
    theirs = [lax.ppermute(t, "c", SWAP) for t in ours]
    return ours, theirs


def layer(tokens_in, gain_attn, w_query, w_keyval, w_out, gain_mlp, w_gate, w_up, w_down):
    core, y_hi, x = lax.axis_index("c"), lax.axis_index("yh"), lax.axis_index("x")
    z_hi, z_lo, y_lo = lax.axis_index("zh"), lax.axis_index("zl"), lax.axis_index("yl")
    block, spot = lax.axis_index(DP), z_lo * 2 + y_lo
    rows, width = tokens_in.shape
    n_dp, n_z = lax.axis_size(DP), lax.axis_size(Z)
    dim = w_query.shape[0]
    block_d = dim // 8
    total = rows * n_dp
    quarter = rows // 4

    gate_next, gate_last = from_x(w_gate, 1), from_x(w_gate, 3)
    up_next, up_last = from_x(w_up, 1), from_x(w_up, 3)
    gate_all = [w_gate, gate_next, from_x(gate_next, 1), gate_last]
    up_all = [w_up, up_next, from_x(up_last, 3), up_last]
    down_next, down_last = from_x(w_down, 1), from_x(w_down, 3)
    down_all = [w_down, down_next, from_x(down_next, 1), down_last]

    ours, theirs = gathered(tokens_in, relative=True)
    place = jnp.stack([core, spot, x, y_hi, z_hi]).astype(jnp.int32)
    gains = gain_attn.astype(F32).reshape(4 * n_z, 1, width)
    pieces = [(t, s, rc) for rc, side in ((0, ours), (1, theirs)) for s, t in enumerate(side)]
    early = [p for p in pieces if p[1] == 0]
    middle = [p for p in pieces if p[1] in (1, 2) and p[2] == 0]
    late = [p for p in pieces if p[1] == 3 or (p[1] != 0 and p[2] == 1)]
    w_kv = w_keyval.T
    sums = project(place, early, gains, w_query, w_kv, None)
    sums = project(place, middle, gains, w_query, w_kv, sums)
    query, kv_part, _ = project(place, late, gains, w_query, w_kv, sums, last=True)

    kv_here = move(
        kv_part.astype(BF16),
        lambda c, zh, zl, **_: {"c": zh // 2, "zh": (zh % 2) * 2 + zl, "zl": c},
    )
    parts = to_all(kv_here, ("yh", "x", "zl", "yl")).reshape(n_dp, 2, HD, rows)
    key_t = jnp.moveaxis(parts[:, 0], 0, 1).reshape(HD, total)
    value_t = jnp.moveaxis(parts[:, 1], 0, 1).reshape(HD, total)

    key_pos = jnp.arange(total, dtype=jnp.int32)
    cos_k, sin_k = rope_tables(key_pos)
    cos_k, sin_k = cos_k.T, sin_k.T
    k1, k2 = key_t[: HD // 2].astype(F32), key_t[HD // 2 :].astype(F32)
    key_rot = jnp.concatenate(
        [k1 * cos_k - k2 * sin_k, k2 * cos_k + k1 * sin_k], axis=0
    ).astype(BF16)
    pos = block * rows + jnp.arange(rows, dtype=jnp.int32)
    cos_q, sin_q = rope_tables(pos)
    heads = w_query.shape[1] // HD
    q_rot = []
    for h in range(heads):
        q1 = query[:, h * HD : h * HD + HD // 2]
        q2 = query[:, h * HD + HD // 2 : (h + 1) * HD]
        q_rot.append(jnp.concatenate([q1 * cos_q - q2 * sin_q, q2 * cos_q + q1 * sin_q], axis=1))
    q_rot = jnp.concatenate(q_rot, axis=0).astype(BF16)
    scores = dot(q_rot, key_rot) * HD ** (-0.5)
    allowed = key_pos[None, :] <= jnp.tile(pos, heads)[:, None]
    scores = jnp.where(allowed, scores, -1e30)
    expo = jnp.exp(scores - jnp.max(scores, axis=-1, keepdims=True))
    probs = (expo / jnp.sum(expo, axis=-1, keepdims=True)).astype(BF16)
    attended = lax.dot_general(
        probs, value_t, (((1,), (1,)), ((), ())), preferred_element_type=F32
    ).astype(BF16)
    sent = lax.ppermute(out_terms(place, attended, w_out, True), "c", SWAP)
    terms = out_terms(place, attended, w_out, False)
    resid = [
        lax.dynamic_slice(t, (x, spot * quarter, 0), (1, quarter, width))[0]
        for t in ours
    ]
    resid = jnp.stack(resid, axis=0)
    resid = jnp.concatenate([pick(resid, j ^ spot) for j in range(4)], axis=1)
    tiles = over_square(terms, sent)
    tiles = exchange(tiles, "zh")
    mid_part = (resid.astype(F32) + tiles.astype(F32).sum(axis=0)).astype(BF16)
    mid_own = move(mid_part, lambda c, yh, **_: {"c": yh, "yh": c})

    ours, theirs = gathered(mid_own)

    gains_mlp = gain_mlp.astype(F32).reshape(n_dp, 1, block_d)
    sent, keep, square = gate_up_terms(place, gains_mlp, ours + theirs, gate_all, up_all)
    sent = lax.ppermute(sent, "yh", SWAP)
    hidden = hidden_units(keep, square, sent, dim)

    other = lax.ppermute(hidden, "yh", SWAP)
    sent = down_terms(place, hidden, other, down_all, True)
    sent = lax.ppermute(sent, "c", SWAP)
    terms = down_terms(place, hidden, other, down_all, False)
    tiles = exchange(over_square(terms, sent), "zh")
    done = (mid_own.astype(F32) + tiles.astype(F32).sum(axis=0)).astype(BF16)
    return move(done, lambda x, zh, **_: {"x": (x + zh) % NX, "zh": x})


def solution(mesh):
    fine = Mesh(mesh.devices.reshape(SIZES), EVERY)
    placed = (
        P(DP, GROUP),
        P(),
        P(None, GROUP),
        P(None, GROUP),
        P(GROUP, None),
        P(),
        P(DP, GROUP),
        P(DP, GROUP),
        P(GROUP, DP),
    )
    return jax.shard_map(layer, mesh=fine, in_specs=placed, out_specs=P(GROUP, DP), check_vma=False)
```
